256 devices in a mesh: px: 4 (over x_lo, core), py: 8 (over y, x_hi), pz: 8 (over z).
Axes of the slice: x: 4 (x_hi: 2, x_lo: 2; x = x_hi * 2 + x_lo), y: 4, z: 8, core: 2. Of those that a mesh axis runs over, the one named last changes fastest.
Arguments:
- control_values: float32 [28, 56, 56, 512], P('px', 'py', 'pz'), may hold values from -6 to 6
- metric_diag: float32 [3, 32, 4096], P(None, 'px', ('py', 'pz')), may hold values from 0.5 to 2
- metric_off: float32 [3, 32, 4096], P(None, 'px', ('py', 'pz')), may hold values from -0.2 to 0.2
- mass_weight: float32 [32, 4096], P('px', ('py', 'pz')), may hold values from 0.5 to 2
- orient: int32 [4, 8, 8, 3], P('px', 'py', 'pz'), may hold values from 0 to 1
Outputs:
- stiffness_out: float32 [28, 56, 56, 512], P('px', 'py', 'pz')
- mass_out: float32 [28, 56, 56, 512], P('px', 'py', 'pz')
The draws below stay inside these ranges and needn't reach their ends.
All inputs are finite; a program needn't handle non-finite values.
Results may differ from the reference program's by a relative error of at most 0.0003.
Values sent between devices are 32-bit elements; how exact they have to be, the bound alone decides.
A program may use at most 64 MiB of HBM per device.

```python
import math
import jax
import jax.numpy as jnp
import numpy as np
from jax import lax

ELEMS = 4
VECS = 512
CTRL = 7
QUAD = 8
N_PX = 4
N_PY = 8
N_PZ = 8


def touch_ends(drawn, own_key, smallest, top_value):
    shape = drawn.shape
    index_at = [jax.random.randint(jax.random.fold_in(own_key, axis), (), 0, shape[axis]) for axis in range(len(shape))]
    drawn = drawn.at[tuple(index_at)].set(smallest)
    longest = shape.index(max(shape))
    index_at[longest] = (index_at[longest] + 1) % shape[longest]
    return drawn.at[tuple(index_at)].set(top_value)


def levels(rng, dims, split, least, high):
    loudness = 1.0
    for axis_at, blocks in split:
        draws = jax.random.uniform(jax.random.fold_in(jax.random.fold_in(rng, 6), axis_at), (blocks,), jnp.float32, least / len(split), high / len(split))
        loudness = loudness * jnp.repeat(jnp.exp(draws), dims[axis_at] // blocks).reshape((-1,) + (1,) * (len(dims) - 1 - axis_at))
    return loudness


def bell_draw(stream_key, shape, deviation, most, split=(), held_as=jnp.bfloat16):
    result = deviation * jax.random.normal(stream_key, shape, jnp.float32)
    if split:
        result = result * levels(stream_key, shape, split, -0.22, 0.18)
    return jnp.clip(result, -most, most).astype(held_as)


def setup_inputs(seed: int = 0) -> dict:
    key_of = jax.random.split(jax.random.key(seed), 6)
    return {
        "control_values": bell_draw(key_of[0], (N_PX * CTRL, N_PY * CTRL, N_PZ * CTRL, VECS), 1.0, 6.0, ((0, 4), (1, 8), (2, 8)), jnp.float32),
        "metric_diag": jnp.clip(jnp.exp(math.log(2.0) - 1.3862944 * jax.random.uniform(key_of[1], (3, N_PX * QUAD, N_PY * N_PZ * QUAD * QUAD), jnp.float32) ** levels(key_of[1], (3, N_PX * QUAD, N_PY * N_PZ * QUAD * QUAD), ((1, 4), (2, 64)), -0.2, 0.2)), 0.5, 2.0),
        "metric_off": jnp.clip(jax.random.uniform(key_of[2], (3, N_PX * QUAD, N_PY * N_PZ * QUAD * QUAD), jnp.float32, -0.2, 0.2) * levels(key_of[2], (3, N_PX * QUAD, N_PY * N_PZ * QUAD * QUAD), ((1, 4), (2, 64)), -0.4, 0.0), -0.2, 0.2),
        "mass_weight": jnp.clip(jnp.exp(math.log(2.0) - 1.3862944 * jax.random.uniform(key_of[3], (N_PX * QUAD, N_PY * N_PZ * QUAD * QUAD), jnp.float32) ** levels(key_of[3], (N_PX * QUAD, N_PY * N_PZ * QUAD * QUAD), ((0, 4), (1, 64)), -0.2, 0.2)), 0.5, 2.0),
        "orient": touch_ends(jax.random.randint(key_of[4], (N_PX, N_PY, N_PZ, 3), 0, 2), jax.random.fold_in(key_of[4], 1), 0, 1).astype(jnp.int32),
    }


def spline_tables(elements):
    knot_row = np.concatenate([np.zeros(3), np.arange(elements + 1) * 1.0, np.full(3, float(elements))])
    offsets = np.array([0.5 - 0.5 / math.sqrt(3.0), 0.5 + 0.5 / math.sqrt(3.0)])
    points = (np.arange(elements)[:, None] + offsets[None, :]).reshape(-1)
    intervals = np.repeat(np.arange(elements), 2) + 3
    current = np.zeros((points.size, knot_row.size - 1))
    current[np.arange(points.size), intervals] = 1.0
    previous = current
    for degree in range(1, 4):
        columns = knot_row.size - 1 - degree
        updated = np.zeros((points.size, columns))
        for i in range(columns):
            lower_gap = knot_row[i + degree] - knot_row[i]
            upper_gap = knot_row[i + degree + 1] - knot_row[i + 1]
            if lower_gap > 0:
                updated[:, i] += (points - knot_row[i]) / lower_gap * current[:, i]
            if upper_gap > 0:
                updated[:, i] += (knot_row[i + degree + 1] - points) / upper_gap * current[:, i + 1]
        previous = current
        current = updated
    slopes = np.zeros(current.shape)
    for i in range(current.shape[1]):
        lower_gap = knot_row[i + 3] - knot_row[i]
        upper_gap = knot_row[i + 4] - knot_row[i + 1]
        if lower_gap > 0:
            slopes[:, i] += 3.0 / lower_gap * previous[:, i]
        if upper_gap > 0:
            slopes[:, i] -= 3.0 / upper_gap * previous[:, i + 1]
    return (current.astype(np.float32), slopes.astype(np.float32))

def contract(pattern, operand, table_part):
    return jnp.einsum(pattern, operand, table_part, precision=lax.Precision.HIGHEST)

def forward_parts(coeffs, values, slopes):
    along_b = contract('ijkv,ck->ijcv', coeffs, values)
    along_d = contract('ijkv,ck->ijcv', coeffs, slopes)
    plain = contract('ijcv,bj->ibcv', along_b, values)
    slope_y = contract('ijcv,bj->ibcv', along_b, slopes)
    slope_z = contract('ijcv,bj->ibcv', along_d, values)
    return (plain, slope_y, slope_z)

def stiffness_apply(parts, diag_terms, off_terms, values, slopes, block_rows):
    plain, slope_y, slope_z = parts
    quad_count = values.shape[0]
    back_x = jnp.zeros(plain.shape, jnp.float32)
    back_y = jnp.zeros(plain.shape, jnp.float32)
    back_z = jnp.zeros(plain.shape, jnp.float32)
    for first_row in range(0, quad_count, block_rows):
        last_row = first_row + block_rows
        slope_rows = slopes[first_row:last_row]
        value_rows = values[first_row:last_row]
        grad_x = contract('ibcv,ai->abcv', plain, slope_rows)
        grad_y = contract('ibcv,ai->abcv', slope_y, value_rows)
        grad_z = contract('ibcv,ai->abcv', slope_z, value_rows)
        diag_rows = diag_terms[:, first_row:last_row, :, :, None]
        off_rows = off_terms[:, first_row:last_row, :, :, None]
        flux_x = diag_rows[0] * grad_x + off_rows[0] * grad_y + off_rows[1] * grad_z
        flux_y = off_rows[0] * grad_x + diag_rows[1] * grad_y + off_rows[2] * grad_z
        flux_z = off_rows[1] * grad_x + off_rows[2] * grad_y + diag_rows[2] * grad_z
        back_x = back_x + contract('abcv,ai->ibcv', flux_x, slope_rows)
        back_y = back_y + contract('abcv,ai->ibcv', flux_y, value_rows)
        back_z = back_z + contract('abcv,ai->ibcv', flux_z, value_rows)
    middle_b = contract('ibcv,bj->ijcv', back_x, values) + contract('ibcv,bj->ijcv', back_y, slopes)
    middle_d = contract('ibcv,bj->ijcv', back_z, values)
    return contract('ijcv,ck->ijkv', middle_b, values) + contract('ijcv,ck->ijkv', middle_d, slopes)

def mass_apply(plain, weights, values, block_rows):
    quad_count = values.shape[0]
    back_mass = jnp.zeros(plain.shape, jnp.float32)
    for first_row in range(0, quad_count, block_rows):
        last_row = first_row + block_rows
        value_rows = values[first_row:last_row]
        point_values = contract('ibcv,ai->abcv', plain, value_rows)
        weighted = weights[first_row:last_row, :, :, None] * point_values
        back_mass = back_mass + contract('abcv,ai->ibcv', weighted, value_rows)
    middle = contract('ibcv,bj->ijcv', back_mass, values)
    return contract('ijcv,ck->ijkv', middle, values)

def flip_frame(grid_data, flip_flags, first_dim):
    for d in range(3):
        grid_data = jnp.where(flip_flags[d] == 1, jnp.flip(grid_data, axis=first_dim + d), grid_data)
    return grid_data

def fold_axis(grid_data, patch_axis, point_axis):
    extent = grid_data.shape[point_axis]
    first_plane = lax.slice_in_dim(grid_data, 0, 1, axis=point_axis)
    last_plane = lax.slice_in_dim(grid_data, extent - 1, extent, axis=point_axis)
    middle = lax.slice_in_dim(grid_data, 1, extent - 1, axis=point_axis)
    from_before = jnp.roll(last_plane, 1, axis=patch_axis)
    from_after = jnp.roll(first_plane, -1, axis=patch_axis)
    return jnp.concatenate([first_plane + from_before, middle, last_plane + from_after], axis=point_axis)

def reference(control_values, metric_diag, metric_off, mass_weight, orient):
    values_np, slopes_np = spline_tables(ELEMS)
    values = jnp.asarray(values_np)
    slopes = jnp.asarray(slopes_np)
    patches = N_PX * N_PY * N_PZ
    coeffs = control_values.reshape(N_PX, CTRL, N_PY, CTRL, N_PZ, CTRL, VECS)
    coeffs = coeffs.transpose(0, 2, 4, 1, 3, 5, 6).reshape(patches, CTRL, CTRL, CTRL, VECS)
    diag_all = metric_diag.reshape(3, N_PX, QUAD, N_PY, N_PZ, QUAD, QUAD)
    diag_all = diag_all.transpose(1, 3, 4, 0, 2, 5, 6).reshape(patches, 3, QUAD, QUAD, QUAD)
    off_all = metric_off.reshape(3, N_PX, QUAD, N_PY, N_PZ, QUAD, QUAD)
    off_all = off_all.transpose(1, 3, 4, 0, 2, 5, 6).reshape(patches, 3, QUAD, QUAD, QUAD)
    weight_all = mass_weight.reshape(N_PX, QUAD, N_PY, N_PZ, QUAD, QUAD)
    weight_all = weight_all.transpose(0, 2, 3, 1, 4, 5).reshape(patches, QUAD, QUAD, QUAD)
    flag_all = orient.reshape(patches, 3)

    def one_patch(patch_items):
        coeff_patch, diag_patch, off_patch, weight_patch, flag_patch = patch_items
        parts = forward_parts(coeff_patch, values, slopes)
        stiffness = stiffness_apply(parts, diag_patch, off_patch, values, slopes, QUAD)
        mass_part = mass_apply(parts[0], weight_patch, values, QUAD)
        return (flip_frame(stiffness, flag_patch, 0), flip_frame(mass_part, flag_patch, 0))
    stiffness_all, mass_all = lax.map(one_patch, (coeffs, diag_all, off_all, weight_all, flag_all))

    def assemble(grid_data):
        grid_data = grid_data.reshape(N_PX, N_PY, N_PZ, CTRL, CTRL, CTRL, VECS)
        grid_data = fold_axis(grid_data, 0, 3)
        grid_data = fold_axis(grid_data, 1, 4)
        grid_data = fold_axis(grid_data, 2, 5)
        return grid_data.reshape(patches, CTRL, CTRL, CTRL, VECS)

    def flip_back(patch_items):
        stiff_patch, mass_patch, flag_patch = patch_items
        return (flip_frame(stiff_patch, flag_patch, 0), flip_frame(mass_patch, flag_patch, 0))
    stiffness_all, mass_all = lax.map(flip_back, (assemble(stiffness_all), assemble(mass_all), flag_all))

    def to_layout(grid_data):
        grid_data = grid_data.reshape(N_PX, N_PY, N_PZ, CTRL, CTRL, CTRL, VECS)
        return grid_data.transpose(0, 3, 1, 4, 2, 5, 6).reshape(N_PX * CTRL, N_PY * CTRL, N_PZ * CTRL, VECS)
    return (to_layout(stiffness_all), to_layout(mass_all))
```

```python
import functools
import math

import jax
import jax.numpy as jnp
import numpy as np
from jax import lax
from jax.experimental import pallas as pl
from jax.experimental.pallas import tpu as pltpu
from jax.sharding import PartitionSpec as P

MESH = pl.DeviceIdType.MESH
LANES = 128
F32 = jnp.float32
BF16 = jnp.bfloat16


def spline_tables(elements):
    knot_row = np.concatenate(
        [np.zeros(3), np.arange(elements + 1) * 1.0, np.full(3, float(elements))]
    )
    offsets = np.array([0.5 - 0.5 / math.sqrt(3.0), 0.5 + 0.5 / math.sqrt(3.0)])
    points = (np.arange(elements)[:, None] + offsets[None, :]).reshape(-1)
    intervals = np.repeat(np.arange(elements), 2) + 3
    current = np.zeros((points.size, knot_row.size - 1))
    current[np.arange(points.size), intervals] = 1.0
    previous = current
    for degree in range(1, 4):
        columns = knot_row.size - 1 - degree
        updated = np.zeros((points.size, columns))
        for i in range(columns):
            lower_gap = knot_row[i + degree] - knot_row[i]
            upper_gap = knot_row[i + degree + 1] - knot_row[i + 1]
            if lower_gap > 0:
                updated[:, i] += (points - knot_row[i]) / lower_gap * current[:, i]
            if upper_gap > 0:
                updated[:, i] += (knot_row[i + degree + 1] - points) / upper_gap * current[:, i + 1]
        previous = current
        current = updated
    slopes = np.zeros(current.shape)
    for i in range(current.shape[1]):
        lower_gap = knot_row[i + 3] - knot_row[i]
        upper_gap = knot_row[i + 4] - knot_row[i + 1]
        if lower_gap > 0:
            slopes[:, i] += 3.0 / lower_gap * previous[:, i]
        if upper_gap > 0:
            slopes[:, i] -= 3.0 / upper_gap * previous[:, i + 1]
    return (current.astype(np.float32), slopes.astype(np.float32))


def split(table):
    high = table.astype(np.float32).astype(BF16)
    low = (table.astype(np.float32) - high.astype(np.float32)).astype(BF16)
    return np.asarray(high), np.asarray(low)


def pair_table(first, second):
    wide_first = np.zeros((8, 8))
    wide_first[:, :7] = first
    wide_second = np.zeros((8, 8))
    wide_second[:, :7] = second
    return np.einsum("bj,ck->bcjk", wide_first, wide_second).reshape(64, 64)


def mirrored(table, flip_j, flip_k):
    grid = table.reshape(64, 8, 8).copy()
    if flip_j:
        grid[:, :7] = grid[:, 6::-1]
    if flip_k:
        grid[:, :, :7] = grid[:, :, 6::-1]
    return grid.reshape(64, 64)


def matmul_tables(values, slopes):
    value_value = pair_table(values, values)
    slope_value = pair_table(slopes, values)
    value_slope = pair_table(values, slopes)
    high, low = split(np.concatenate([value_value, slope_value, value_slope]))
    forward = np.concatenate([high, low, high], axis=1)
    back_mixed, back_plain = [], []
    for flips in range(4):
        vv, sv, vs = (
            split(mirrored(t, flips // 2, flips % 2).T) for t in (value_value, slope_value, value_slope)
        )
        none = np.zeros((64, 64), vv[0].dtype)
        mixed = np.concatenate([sv[0], vs[0]], axis=1)
        mixed_low = np.concatenate([sv[1], vs[1], none, none], axis=1)
        back_mixed.append(np.concatenate([np.concatenate([mixed, mixed], axis=1), mixed_low]))
        back_plain.append(
            np.concatenate(
                [
                    np.concatenate([vv[0], vv[0], none, none], axis=1),
                    np.concatenate([vv[1], none, none, none], axis=1),
                    np.concatenate([none, none, vv[0], vv[0]], axis=1),
                    np.concatenate([none, none, vv[1], none], axis=1),
                ]
            )
        )
    return forward, np.stack(back_mixed), np.stack(back_plain)


def halves(x):
    high = x.astype(BF16)
    low = (x - high.astype(F32)).astype(BF16)
    return high, low


def mac(terms):
    total = None
    for coefficient, x in terms:
        part = x * float(coefficient)
        total = part if total is None else total + part
    return total


def kernel(
    values, slopes, tiles,
    control, diag, off, weight, orient, forward, mixed, plain,
    stiff_out, mass_out,
    ubuf, gbuf, planes, metric, scales, staged,
    xrecv, yrecv, zsend, zrecv,
    load_sem, out_sem, send_sem, recv_sem,
):
    px, py, pz = (lax.axis_index(a) for a in ("px", "py", "pz"))
    nx, ny, nz = (lax.axis_size(a) for a in ("px", "py", "pz"))
    x_up, x_down = lax.rem(px + 1, nx), lax.rem(px + nx - 1, nx)
    y_up, y_down = lax.rem(py + 1, ny), lax.rem(py + ny - 1, ny)
    z_up, z_down = lax.rem(pz + 1, nz), lax.rem(pz + nz - 1, nz)
    x_mirror = nx - 1 - px
    odd = lax.rem(px, 2)
    rim, first = 6 * odd, 1 - odd

    barrier = pltpu.get_barrier_semaphore()
    for device in (
        (x_up, py, pz), (x_down, py, pz),
        (px, y_up, pz), (px, y_down, pz), (x_mirror, y_up, pz), (x_mirror, y_down, pz),
        (px, py, z_up), (px, py, z_down),
    ):
        pl.semaphore_signal(barrier, inc=1, device_id=device, device_id_type=MESH)

    def load(t):
        return pltpu.make_async_copy(
            control.at[:, :, :, pl.ds(pl.multiple_of(t * LANES, LANES), LANES)],
            ubuf.at[t, :, :, pl.ds(0, 7), :],
            load_sem.at[t],
        )

    for t in range(tiles):
        load(t).start()
    pad = jnp.zeros((7, 7, 1, LANES), F32)
    for t in range(tiles):
        ubuf[t, :, :, pl.ds(7, 1), :] = pad

    flip_i, flip_j, flip_k = (orient[0, 0, 0, d] for d in range(3))
    variant = 2 * flip_j + flip_k

    scales[pl.ds(0, 24), pl.ds(0, 64)] = diag[...].reshape(24, 64)
    scales[pl.ds(24, 24), pl.ds(0, 64)] = off[...].reshape(24, 64)
    scales[pl.ds(48, 8), pl.ds(0, 64)] = weight[...]
    turned = scales[...].T
    for m in range(56):
        metric[m] = jnp.broadcast_to(turned[:64, m : m + 1], (64, LANES))

    def compute(t):
        load(t).wait()
        forward_table = forward[...]
        mixed_table = mixed[variant]
        plain_table = plain[variant]
        nothing = jnp.zeros((8, LANES), F32)
        for e in range(4):
            source = [ubuf[t, i].reshape(56, LANES) for i in range(e, e + 4)]
            value_cat, slope_cat = [], []
            for a in (2 * e, 2 * e + 1):
                for table, cat in ((values, value_cat), (slopes, slope_cat)):
                    x = mac([(table[a, e + n], source[n]) for n in range(4)])
                    high, low = halves(jnp.concatenate([x, nothing], axis=0))
                    cat.append(jnp.concatenate([high, high, low], axis=0))
            at_values = jnp.dot(
                forward_table, jnp.concatenate(value_cat, axis=1), preferred_element_type=F32
            )
            at_slopes = jnp.dot(
                forward_table[:64], jnp.concatenate(slope_cat, axis=1), preferred_element_type=F32
            )
            mixed_in, plain_in = [], []
            for n, a in enumerate((2 * e, 2 * e + 1)):
                lanes = slice(n * LANES, (n + 1) * LANES)
                p, g2, g3 = (at_values[64 * r : 64 * r + 64, lanes] for r in range(3))
                g1 = at_slopes[:, lanes]
                d0, d1, d2, o0, o1, o2, w = (metric[8 * s + a] for s in range(7))
                f1 = d0 * g1 + o0 * g2 + o1 * g3
                f2 = o0 * g1 + d1 * g2 + o2 * g3
                f3 = o1 * g1 + o2 * g2 + d2 * g3
                f1h, f1l = halves(f1)
                f2h, f2l = halves(f2)
                f3h, f3l = halves(f3)
                mh, ml = halves(w * p)
                mixed_in.append(jnp.concatenate([f2h, f3h, f2l, f3l], axis=0))
                plain_in.append(jnp.concatenate([f1h, f1l, mh, ml], axis=0))
            mixed_back = jnp.dot(
                mixed_table, jnp.concatenate(mixed_in, axis=1), preferred_element_type=F32
            )
            plain_back = jnp.dot(
                plain_table, jnp.concatenate(plain_in, axis=1), preferred_element_type=F32
            )
            terms = []
            for n in range(2):
                lanes = slice(n * LANES, (n + 1) * LANES)
                terms.append(
                    (
                        plain_back[0:56, lanes] + plain_back[64:120, lanes],
                        mixed_back[0:56, lanes] + mixed_back[64:120, lanes],
                        plain_back[128:184, lanes] + plain_back[192:248, lanes],
                    )
                )
            for i in range(e, e + 4):
                stiff = mac(
                    [(slopes[2 * e + n, i], terms[n][0]) for n in range(2)]
                    + [(values[2 * e + n, i], terms[n][1]) for n in range(2)]
                )
                mass = mac([(values[2 * e + n, i], terms[n][2]) for n in range(2)])
                if e > 0 and i < e + 3:
                    stiff = stiff + planes[0, i]
                    mass = mass + planes[1, i]
                planes[0, i] = stiff
                planes[1, i] = mass
        for o in range(2):
            for i in range(7):
                gbuf[o, t, i] = planes[o, i + flip_i * (6 - 2 * i)].reshape(7, 8, LANES)

    def remote(t, which, src, dst, device):
        return pltpu.make_async_remote_copy(
            src_ref=src, dst_ref=dst, send_sem=send_sem.at[t, which], recv_sem=recv_sem.at[t, which],
            device_id=device, device_id_type=MESH,
        )

    rows = pl.ds(0, 7)

    def x_copies(t):
        return [
            remote(t, 0, gbuf.at[:, t, 6, :, rows, :], xrecv.at[t, 0, :, :, rows, :], (x_up, py, pz)),
            remote(t, 1, gbuf.at[:, t, 0, :, rows, :], xrecv.at[t, 1, :, :, rows, :], (x_down, py, pz)),
        ]

    def y_copies(t):
        inner = pl.ds(first, 6)
        return [
            remote(t, 2, gbuf.at[:, t, inner, 6, rows, :], yrecv.at[t, 0, :, inner, rows, :], (px, y_up, pz)),
            remote(t, 3, gbuf.at[:, t, inner, 0, rows, :], yrecv.at[t, 1, :, inner, rows, :], (px, y_down, pz)),
            remote(t, 4, gbuf.at[:, t, rim, 6, rows, :], yrecv.at[t, 0, :, 6 - rim, rows, :], (x_mirror, y_up, pz)),
            remote(t, 5, gbuf.at[:, t, rim, 0, rows, :], yrecv.at[t, 1, :, 6 - rim, rows, :], (x_mirror, y_down, pz)),
        ]

    def z_copies(t):
        return [
            remote(t, 6, zsend.at[t, 1], zrecv.at[t, 0], (px, py, z_up)),
            remote(t, 7, zsend.at[t, 0], zrecv.at[t, 1], (px, py, z_down)),
        ]

    def start(copies):
        for c in copies:
            c.start()

    def wait(copies):
        for c in copies:
            c.wait()

    def fold_x(t):
        for side in range(2):
            for o in range(2):
                gbuf[o, t, 6 * side, :, rows, :] = (
                    gbuf[o, t, 6 * side, :, rows, :] + xrecv[t, side, o, :, rows, :]
                )

    def fold_y(t):
        for side in range(2):
            for o in range(2):
                gbuf[o, t, :, 6 * side, rows, :] = (
                    gbuf[o, t, :, 6 * side, rows, :] + yrecv[t, side, o, :, rows, :]
                )

    def take_z(t):
        for side in range(2):
            for o in range(2):
                for i in range(7):
                    zsend[t, side, o, i] = gbuf[o, t, i, :, 6 * side, :]

    def fold_z(t):
        for side in range(2):
            for o in range(2):
                for i in range(7):
                    gbuf[o, t, i, :, 6 * side, :] = gbuf[o, t, i, :, 6 * side, :] + zrecv[t, side, o, i]

    sublane = lax.broadcasted_iota(jnp.int32, (8, LANES), 0)
    turned_rows = jnp.where(sublane < 7, 6 - sublane, sublane)
    pick = sublane + flip_k * (turned_rows - sublane)

    def out_copies(t):
        lanes = pl.ds(pl.multiple_of(t * LANES, LANES), LANES)
        return [
            pltpu.make_async_copy(staged.at[o, t, :, :, rows, :], out.at[:, :, :, lanes], out_sem.at[o, t])
            for o, out in enumerate((stiff_out, mass_out))
        ]

    def finish(t):
        for o in range(2):
            for i in range(7):
                for j in range(7):
                    tile = gbuf[o, t, i + flip_i * (6 - 2 * i), j + flip_j * (6 - 2 * j)]
                    staged[o, t, i, j] = jnp.take_along_axis(tile, pick, axis=0)
        start(out_copies(t))

    def step(s, carry):
        @pl.when(s < tiles)
        def _():
            compute(s)

            @pl.when(s == 0)
            def _():
                pl.semaphore_wait(barrier, 8)

            start(x_copies(s))

        @pl.when(jnp.logical_and(s >= 1, s < tiles + 1))
        def _():
            wait(x_copies(s - 1))
            fold_x(s - 1)
            start(y_copies(s - 1))

        @pl.when(jnp.logical_and(s >= 2, s < tiles + 2))
        def _():
            wait(y_copies(s - 2))
            fold_y(s - 2)
            take_z(s - 2)
            start(z_copies(s - 2))

        @pl.when(s >= 3)
        def _():
            wait(z_copies(s - 3))
            fold_z(s - 3)
            finish(s - 3)

        return carry

    lax.fori_loop(0, tiles + 3, step, 0)
    for t in range(tiles):
        wait(out_copies(t))


def per_device(control_values, metric_diag, metric_off, mass_weight, orient):
    values, slopes = spline_tables(4)
    tiles = control_values.shape[-1] // LANES
    forward, mixed, plain = (jnp.asarray(t) for t in matmul_tables(values, slopes))
    shape = jax.ShapeDtypeStruct(control_values.shape, F32)
    in_vmem = pl.BlockSpec(memory_space=pltpu.VMEM)
    anywhere = pl.BlockSpec(memory_space=pl.ANY)
    return pl.pallas_call(
        functools.partial(kernel, values, slopes, tiles),
        out_shape=(shape, shape),
        in_specs=[anywhere, in_vmem, in_vmem, in_vmem, pl.BlockSpec(memory_space=pltpu.SMEM)] + [in_vmem] * 3,
        out_specs=(anywhere, anywhere),
        scratch_shapes=[
            pltpu.VMEM((tiles, 7, 7, 8, LANES), F32),
            pltpu.VMEM((2, tiles, 7, 7, 8, LANES), F32),
            pltpu.VMEM((2, 7, 56, LANES), F32),
            pltpu.VMEM((56, 64, LANES), F32),
            pltpu.VMEM((128, 128), F32),
            pltpu.VMEM((2, tiles, 7, 7, 8, LANES), F32),
            pltpu.VMEM((tiles, 2, 2, 7, 8, LANES), F32),
            pltpu.VMEM((tiles, 2, 2, 7, 8, LANES), F32),
            pltpu.VMEM((tiles, 2, 2, 7, 7, LANES), F32),
            pltpu.VMEM((tiles, 2, 2, 7, 7, LANES), F32),
            pltpu.SemaphoreType.DMA((tiles,)),
            pltpu.SemaphoreType.DMA((2, tiles)),
            pltpu.SemaphoreType.DMA((tiles, 8)),
            pltpu.SemaphoreType.DMA((tiles, 8)),
        ],
        compiler_params=pltpu.CompilerParams(
            collective_id=0, has_side_effects=True, vmem_limit_bytes=40 * 1024 * 1024
        ),
        name="apply",
    )(control_values, metric_diag, metric_off, mass_weight, orient, forward, mixed, plain)


def solution(mesh):
    in_specs = (
        P("px", "py", "pz", None),
        P(None, "px", ("py", "pz")),
        P(None, "px", ("py", "pz")),
        P("px", ("py", "pz")),
        P("px", "py", "pz", None),
    )
    out_specs = (P("px", "py", "pz", None), P("px", "py", "pz", None))
    return jax.shard_map(
        per_device, mesh=mesh, in_specs=in_specs, out_specs=out_specs, check_vma=False
    )
```

```python
import functools
import math

import jax
import jax.numpy as jnp
import numpy as np
from jax import lax
from jax.experimental import pallas as pl
from jax.experimental.pallas import tpu as pltpu
from jax.sharding import PartitionSpec as P

MESH = pl.DeviceIdType.MESH
LANES = 128
F32 = jnp.float32
BF16 = jnp.bfloat16


def spline_tables(elements):
    knot_row = np.concatenate(
        [np.zeros(3), np.arange(elements + 1) * 1.0, np.full(3, float(elements))]
    )
    offsets = np.array([0.5 - 0.5 / math.sqrt(3.0), 0.5 + 0.5 / math.sqrt(3.0)])
    points = (np.arange(elements)[:, None] + offsets[None, :]).reshape(-1)
    intervals = np.repeat(np.arange(elements), 2) + 3
    current = np.zeros((points.size, knot_row.size - 1))
    current[np.arange(points.size), intervals] = 1.0
    previous = current
    for degree in range(1, 4):
        columns = knot_row.size - 1 - degree
        updated = np.zeros((points.size, columns))
        for i in range(columns):
            lower_gap = knot_row[i + degree] - knot_row[i]
            upper_gap = knot_row[i + degree + 1] - knot_row[i + 1]
            if lower_gap > 0:
                updated[:, i] += (points - knot_row[i]) / lower_gap * current[:, i]
            if upper_gap > 0:
                updated[:, i] += (knot_row[i + degree + 1] - points) / upper_gap * current[:, i + 1]
        previous = current
        current = updated
    slopes = np.zeros(current.shape)
    for i in range(current.shape[1]):
        lower_gap = knot_row[i + 3] - knot_row[i]
        upper_gap = knot_row[i + 4] - knot_row[i + 1]
        if lower_gap > 0:
            slopes[:, i] += 3.0 / lower_gap * previous[:, i]
        if upper_gap > 0:
            slopes[:, i] -= 3.0 / upper_gap * previous[:, i + 1]
    return (current.astype(np.float32), slopes.astype(np.float32))


def split(table):
    high = table.astype(np.float32).astype(BF16)
    low = (table.astype(np.float32) - high.astype(np.float32)).astype(BF16)
    return np.asarray(high), np.asarray(low)


def pair_table(first, second):
    wide_first = np.zeros((8, 8))
    wide_first[:, :7] = first
    wide_second = np.zeros((8, 8))
    wide_second[:, :7] = second
    return np.einsum("bj,ck->bcjk", wide_first, wide_second).reshape(64, 64)


def mirrored(table, flip_j, flip_k):
    grid = table.reshape(64, 8, 8).copy()
    if flip_j:
        grid[:, :7] = grid[:, 6::-1]
    if flip_k:
        grid[:, :, :7] = grid[:, :, 6::-1]
    return grid.reshape(64, 64)


def matmul_tables(values, slopes):
    value_value = pair_table(values, values)
    slope_value = pair_table(slopes, values)
    value_slope = pair_table(values, slopes)
    high, low = split(np.concatenate([value_value, slope_value, value_slope]))
    forward = np.concatenate([high, low, high], axis=1)
    back_mixed, back_plain = [], []
    for flips in range(4):
        vv, sv, vs = (
            split(mirrored(t, flips // 2, flips % 2).T) for t in (value_value, slope_value, value_slope)
        )
        none = np.zeros((64, 64), vv[0].dtype)
        mixed = np.concatenate([sv[0], vs[0]], axis=1)
        mixed_low = np.concatenate([sv[1], vs[1], none, none], axis=1)
        back_mixed.append(np.concatenate([np.concatenate([mixed, mixed], axis=1), mixed_low]))
        back_plain.append(
            np.concatenate(
                [
                    np.concatenate([vv[0], vv[0], none, none], axis=1),
                    np.concatenate([vv[1], none, none, none], axis=1),
                    np.concatenate([none, none, vv[0], vv[0]], axis=1),
                    np.concatenate([none, none, vv[1], none], axis=1),
                ]
            )
        )
    return forward, np.stack(back_mixed), np.stack(back_plain)


def halves(x):
    high = x.astype(BF16)
    low = (x - high.astype(F32)).astype(BF16)
    return high, low


def mac(terms):
    total = None
    for coefficient, x in terms:
        part = x * float(coefficient)
        total = part if total is None else total + part
    return total


def kernel(
    values, slopes, tiles,
    control, diag_in, off_in, weight_in, orient_in, forward_in, mixed_in_hbm, plain_in_hbm,
    stiff_out, mass_out,
    diag, off, weight, orient, forward, mixed, plain,
    ubuf, gbuf, planes, metric, scales,
    xrecv, ysend_inner, yrecv_inner, ysend_ends, yrecv_ends, yrecv_sides,
    zsend_inner, zrecv_inner, zsend_sides, zrecv_sides,
    load_sem, small_sem, send_sem, recv_sem,
):
    px, py, pz = (lax.axis_index(a) for a in ("px", "py", "pz"))
    nx, ny, nz = (lax.axis_size(a) for a in ("px", "py", "pz"))
    x_up, x_down = lax.rem(px + 1, nx), lax.rem(px + nx - 1, nx)
    y_up, y_down = lax.rem(py + 1, ny), lax.rem(py + ny - 1, ny)
    z_up, z_down = lax.rem(pz + 1, nz), lax.rem(pz + nz - 1, nz)
    x_mirror = nx - 1 - px
    odd = lax.rem(px, 2)
    rim = 6 * odd

    barrier = pltpu.get_barrier_semaphore()
    for device in (
        (x_up, py, pz), (x_down, py, pz),
        (px, y_up, pz), (px, y_down, pz), (x_mirror, y_up, pz), (x_mirror, y_down, pz),
        (px, py, z_up), (px, py, z_down),
    ):
        pl.semaphore_signal(barrier, inc=1, device_id=device, device_id_type=MESH)

    def load(t):
        return pltpu.make_async_copy(
            control.at[:, :, :, pl.ds(pl.multiple_of(t * LANES, LANES), LANES)],
            ubuf.at[t, :, :, pl.ds(0, 7), :],
            load_sem.at[t],
        )

    small = [
        pltpu.make_async_copy(src, dst, small_sem.at[n])
        for n, (src, dst) in enumerate(
            (
                (orient_in, orient), (diag_in, diag), (off_in, off), (weight_in, weight),
                (forward_in, forward), (mixed_in_hbm, mixed), (plain_in_hbm, plain),
            )
        )
    ]
    for c in small[:4]:
        c.start()
    load(0).start()
    for c in small[4:]:
        c.start()
    for t in range(1, tiles):
        load(t).start()
    pad = jnp.zeros((7, 7, 1, LANES), F32)
    for t in range(tiles):
        ubuf[t, :, :, pl.ds(7, 1), :] = pad

    for c in small[:4]:
        c.wait()
    flip_i, flip_j, flip_k = (orient[0, 0, 0, d] for d in range(3))
    variant = 2 * flip_j + flip_k

    scales[pl.ds(0, 24), pl.ds(0, 64)] = diag[...].reshape(24, 64)
    scales[pl.ds(24, 24), pl.ds(0, 64)] = off[...].reshape(24, 64)
    scales[pl.ds(48, 8), pl.ds(0, 64)] = weight[...]
    turned = scales[...].T
    for m in range(56):
        metric[m] = jnp.broadcast_to(turned[:64, m : m + 1], (64, LANES))

    for c in small[4:]:
        c.wait()

    def compute(t):
        load(t).wait()
        forward_table = forward[...]
        mixed_table = mixed[variant]
        plain_table = plain[variant]
        nothing = jnp.zeros((8, LANES), F32)
        def ahead(e):
            source = [ubuf[t, i].reshape(56, LANES) for i in range(e, e + 4)]
            value_cat, slope_cat = [], []
            for a in (2 * e, 2 * e + 1):
                for table, cat in ((values, value_cat), (slopes, slope_cat)):
                    x = mac([(table[a, e + n], source[n]) for n in range(4)])
                    high, low = halves(jnp.concatenate([x, nothing], axis=0))
                    cat.append(jnp.concatenate([high, high, low], axis=0))
            at_values = jnp.dot(
                forward_table, jnp.concatenate(value_cat, axis=1), preferred_element_type=F32
            )
            at_slopes = jnp.dot(
                forward_table[:64], jnp.concatenate(slope_cat, axis=1), preferred_element_type=F32
            )
            return at_values, at_slopes

        def back(e, at_values, at_slopes):
            mixed_in, plain_in = [], []
            for n, a in enumerate((2 * e, 2 * e + 1)):
                lanes = slice(n * LANES, (n + 1) * LANES)
                p, g2, g3 = (at_values[64 * r : 64 * r + 64, lanes] for r in range(3))
                g1 = at_slopes[:, lanes]
                d0, d1, d2, o0, o1, o2, w = (metric[8 * s + a] for s in range(7))
                f1 = d0 * g1 + o0 * g2 + o1 * g3
                f2 = o0 * g1 + d1 * g2 + o2 * g3
                f3 = o1 * g1 + o2 * g2 + d2 * g3
                f1h, f1l = halves(f1)
                f2h, f2l = halves(f2)
                f3h, f3l = halves(f3)
                mh, ml = halves(w * p)
                mixed_in.append(jnp.concatenate([f2h, f3h, f2l, f3l], axis=0))
                plain_in.append(jnp.concatenate([f1h, f1l, mh, ml], axis=0))
            mixed_back = jnp.dot(
                mixed_table, jnp.concatenate(mixed_in, axis=1), preferred_element_type=F32
            )
            plain_back = jnp.dot(
                plain_table, jnp.concatenate(plain_in, axis=1), preferred_element_type=F32
            )
            return mixed_back, plain_back

        def gather(e, mixed_back, plain_back):
            terms = []
            for n in range(2):
                lanes = slice(n * LANES, (n + 1) * LANES)
                terms.append(
                    (
                        plain_back[0:56, lanes] + plain_back[64:120, lanes],
                        mixed_back[0:56, lanes] + mixed_back[64:120, lanes],
                        plain_back[128:184, lanes] + plain_back[192:248, lanes],
                    )
                )
            for i in range(e, e + 4):
                stiff = mac(
                    [(slopes[2 * e + n, i], terms[n][0]) for n in range(2)]
                    + [(values[2 * e + n, i], terms[n][1]) for n in range(2)]
                )
                mass = mac([(values[2 * e + n, i], terms[n][2]) for n in range(2)])
                if e > 0 and i < e + 3:
                    stiff = stiff + planes[0, i]
                    mass = mass + planes[1, i]
                planes[0, i] = stiff
                planes[1, i] = mass

        up = {0: ahead(0), 1: ahead(1)}
        down = {}
        for e in range(4):
            down[e] = back(e, *up.pop(e))
            if e + 2 < 4:
                up[e + 2] = ahead(e + 2)
            if e >= 1:
                gather(e - 1, *down.pop(e - 1))
        gather(3, *down.pop(3))
        for o in range(2):
            for i in range(7):
                gbuf[o, t, i] = planes[o, i + flip_i * (6 - 2 * i)].reshape(7, 8, LANES)

    def remote(t, which, src, dst, device):
        return pltpu.make_async_remote_copy(
            src_ref=src, dst_ref=dst, send_sem=send_sem.at[t, which], recv_sem=recv_sem.at[t, which],
            device_id=device, device_id_type=MESH,
        )

    rows = pl.ds(0, 7)

    def x_copies(t):
        return [
            remote(t, 0, gbuf.at[:, t, 6, :, rows, :], xrecv.at[t, 0, :, :, rows, :], (x_up, py, pz)),
            remote(t, 1, gbuf.at[:, t, 0, :, rows, :], xrecv.at[t, 1, :, :, rows, :], (x_down, py, pz)),
        ]

    def y_pair(t, which, sent, received):
        return [
            remote(t, which, sent.at[t, 1], received.at[t, 0], (px, y_up, pz)),
            remote(t, which + 1, sent.at[t, 0], received.at[t, 1], (px, y_down, pz)),
        ]

    def y_inner(t):
        return y_pair(t, 2, ysend_inner, yrecv_inner)

    def y_ends(t):
        return y_pair(t, 4, ysend_ends, yrecv_ends)

    def y_sides(t):
        near = 6 - rim
        there = 1 - odd
        return [
            remote(t, 6, gbuf.at[:, t, near, 6, rows, :], yrecv_sides.at[t, 0, there, :, rows, :], (px, y_up, pz)),
            remote(t, 7, gbuf.at[:, t, near, 0, rows, :], yrecv_sides.at[t, 1, there, :, rows, :], (px, y_down, pz)),
            remote(t, 8, gbuf.at[:, t, rim, 6, rows, :], yrecv_sides.at[t, 0, there, :, rows, :], (x_mirror, y_up, pz)),
            remote(t, 9, gbuf.at[:, t, rim, 0, rows, :], yrecv_sides.at[t, 1, there, :, rows, :], (x_mirror, y_down, pz)),
        ]

    def z_pair(t, which, sent, received):
        return [
            remote(t, which, sent.at[t, 1], received.at[t, 0], (px, py, z_up)),
            remote(t, which + 1, sent.at[t, 0], received.at[t, 1], (px, py, z_down)),
        ]

    def z_inner(t):
        return z_pair(t, 10, zsend_inner, zrecv_inner)

    def z_sides(t):
        return z_pair(t, 12, zsend_sides, zrecv_sides)

    def start(copies):
        for c in copies:
            c.start()

    def wait(copies):
        for c in copies:
            c.wait()

    def fold_x(t):
        for side in range(2):
            for o in range(2):
                gbuf[o, t, 6 * side, :, rows, :] = (
                    gbuf[o, t, 6 * side, :, rows, :] + xrecv[t, side, o, :, rows, :]
                )

    inner_rows = [(i, i - 1) for i in range(1, 6)]
    side_rows = [(6 * n, n) for n in range(2)]

    def take_z(t, sent, where):
        for side in range(2):
            for o in range(2):
                for i, n in where:
                    sent[t, side, o, n] = gbuf[o, t, i, :, 6 * side, :]

    def fold_z(t, received, where):
        for side in range(2):
            for o in range(2):
                for i, n in where:
                    gbuf[o, t, i, :, 6 * side, :] = gbuf[o, t, i, :, 6 * side, :] + received[t, side, o, n]

    mid = pl.ds(1, 5)

    def take_y_inner(t):
        for side in range(2):
            for o in range(2):
                ysend_inner[t, side, o] = gbuf[o, t, mid, 6 * side, mid, :]

    def take_y_ends(t):
        for side in range(2):
            for o in range(2):
                for n in range(2):
                    ysend_ends[t, side, o, n] = gbuf[o, t, mid, 6 * side, 6 * n, :]

    def fold_y(t):
        for side in range(2):
            for o in range(2):
                j = 6 * side
                gbuf[o, t, mid, j, mid, :] = gbuf[o, t, mid, j, mid, :] + yrecv_inner[t, side, o]
                for n in range(2):
                    gbuf[o, t, mid, j, 6 * n, :] = gbuf[o, t, mid, j, 6 * n, :] + yrecv_ends[t, side, o, n]
                    gbuf[o, t, 6 * n, j, rows, :] = gbuf[o, t, 6 * n, j, rows, :] + yrecv_sides[t, side, n, o, rows, :]

    sublane = lax.broadcasted_iota(jnp.int32, (8, LANES), 0)
    turned_rows = jnp.where(sublane < 7, 6 - sublane, sublane)
    pick = sublane + flip_k * (turned_rows - sublane)

    def finish(t):
        lanes = pl.ds(pl.multiple_of(t * LANES, LANES), LANES)
        for o, out in enumerate((stiff_out, mass_out)):
            for i in range(7):
                for j in range(7):
                    tile = gbuf[o, t, i + flip_i * (6 - 2 * i), j + flip_j * (6 - 2 * j)]
                    out[i, j, :, lanes] = jnp.take_along_axis(tile, pick, axis=0)[:7]

    def produce(t, carry):
        compute(t)

        @pl.when(t == 0)
        def _():
            pl.semaphore_wait(barrier, 8)

        start(x_copies(t))
        take_z(t, zsend_inner, inner_rows)
        start(z_inner(t))
        take_y_inner(t)

        @pl.when(t >= 1)
        def _():
            start(y_inner(t - 1))

        return carry

    def after_x(t, carry):
        wait(x_copies(t))
        fold_x(t)
        take_z(t, zsend_sides, side_rows)
        start(z_sides(t))
        return carry

    def after_z(t, carry):
        wait(z_inner(t))
        fold_z(t, zrecv_inner, inner_rows)
        take_y_ends(t)
        start(y_ends(t))
        wait(z_sides(t))
        fold_z(t, zrecv_sides, side_rows)
        start(y_sides(t))
        return carry

    def after_y(t, carry):
        wait(y_inner(t))
        wait(y_ends(t))
        wait(y_sides(t))
        fold_y(t)
        finish(t)
        return carry

    lax.fori_loop(0, tiles, produce, 0)
    start(y_inner(tiles - 1))
    for stage in (after_x, after_z, after_y):
        lax.fori_loop(0, tiles, stage, 0)


def put(stiff, mass, stiff_out, mass_out, sem):
    copies = [
        pltpu.make_async_copy(source.at[i], target.at[i], sem.at[n, i])
        for i in range(7)
        for n, (source, target) in enumerate(((stiff, stiff_out), (mass, mass_out)))
    ]
    for c in copies:
        c.start()
    for c in copies:
        c.wait()


def per_device(control_values, metric_diag, metric_off, mass_weight, orient):
    values, slopes = spline_tables(4)
    tiles = control_values.shape[-1] // LANES
    forward, mixed, plain = (jnp.asarray(t) for t in matmul_tables(values, slopes))
    shape = jax.ShapeDtypeStruct(control_values.shape, F32)
    in_vmem = pl.BlockSpec(memory_space=pltpu.VMEM)
    in_hbm = pl.BlockSpec(memory_space=pltpu.HBM)
    results = pl.pallas_call(
        functools.partial(kernel, values, slopes, tiles),
        out_shape=(pltpu.VMEM(control_values.shape, F32),) * 2,
        in_specs=[in_hbm] * 8,
        out_specs=(in_vmem, in_vmem),
        scratch_shapes=[
            pltpu.VMEM(metric_diag.shape, F32),
            pltpu.VMEM(metric_off.shape, F32),
            pltpu.VMEM(mass_weight.shape, F32),
            pltpu.SMEM(orient.shape, jnp.int32),
            pltpu.VMEM(forward.shape, BF16),
            pltpu.VMEM(mixed.shape, BF16),
            pltpu.VMEM(plain.shape, BF16),
            pltpu.VMEM((tiles, 7, 7, 8, LANES), F32),
            pltpu.VMEM((2, tiles, 7, 7, 8, LANES), F32),
            pltpu.VMEM((2, 7, 56, LANES), F32),
            pltpu.VMEM((56, 64, LANES), F32),
            pltpu.VMEM((128, 128), F32),
            pltpu.VMEM((tiles, 2, 2, 7, 8, LANES), F32),
            pltpu.VMEM((tiles, 2, 2, 5, 5, LANES), F32),
            pltpu.VMEM((tiles, 2, 2, 5, 5, LANES), F32),
            pltpu.VMEM((tiles, 2, 2, 2, 5, LANES), F32),
            pltpu.VMEM((tiles, 2, 2, 2, 5, LANES), F32),
            pltpu.VMEM((tiles, 2, 2, 2, 8, LANES), F32),
            pltpu.VMEM((tiles, 2, 2, 5, 7, LANES), F32),
            pltpu.VMEM((tiles, 2, 2, 5, 7, LANES), F32),
            pltpu.VMEM((tiles, 2, 2, 2, 7, LANES), F32),
            pltpu.VMEM((tiles, 2, 2, 2, 7, LANES), F32),
            pltpu.SemaphoreType.DMA((tiles,)),
            pltpu.SemaphoreType.DMA((7,)),
            pltpu.SemaphoreType.DMA((tiles, 14)),
            pltpu.SemaphoreType.DMA((tiles, 14)),
        ],
        compiler_params=pltpu.CompilerParams(
            collective_id=0, has_side_effects=True, vmem_limit_bytes=40 * 1024 * 1024
        ),
        name="apply",
    )(
        *(
            pltpu.with_memory_space_constraint(x, pltpu.HBM)
            for x in (control_values, metric_diag, metric_off, mass_weight, orient, forward, mixed, plain)
        )
    )
    return pl.pallas_call(
        put,
        out_shape=(shape, shape),
        in_specs=[pl.BlockSpec(memory_space=pl.ANY)] * 2,
        out_specs=(in_hbm, in_hbm),
        scratch_shapes=[pltpu.SemaphoreType.DMA((2, 7))],
        compiler_params=pltpu.CompilerParams(vmem_limit_bytes=1024 * 1024),
        name="put",
    )(*(pltpu.with_memory_space_constraint(x, pltpu.VMEM) for x in results))


def solution(mesh):
    in_specs = (
        P("px", "py", "pz", None),
        P(None, "px", ("py", "pz")),
        P(None, "px", ("py", "pz")),
        P("px", ("py", "pz")),
        P("px", "py", "pz", None),
    )
    out_specs = (P("px", "py", "pz", None), P("px", "py", "pz", None))
    return jax.shard_map(
        per_device, mesh=mesh, in_specs=in_specs, out_specs=out_specs, check_vma=False
    )
```

```python
import functools
import math

import jax
import jax.numpy as jnp
import numpy as np
from jax import lax
from jax.experimental import pallas as pl
from jax.experimental.pallas import tpu as pltpu
from jax.sharding import PartitionSpec as P

MESH = pl.DeviceIdType.MESH
LANES = 128
F32 = jnp.float32
BF16 = jnp.bfloat16


def spline_tables(elements):
    knot_row = np.concatenate(
        [np.zeros(3), np.arange(elements + 1) * 1.0, np.full(3, float(elements))]
    )
    offsets = np.array([0.5 - 0.5 / math.sqrt(3.0), 0.5 + 0.5 / math.sqrt(3.0)])
    points = (np.arange(elements)[:, None] + offsets[None, :]).reshape(-1)
    intervals = np.repeat(np.arange(elements), 2) + 3
    current = np.zeros((points.size, knot_row.size - 1))
    current[np.arange(points.size), intervals] = 1.0
    previous = current
    for degree in range(1, 4):
        columns = knot_row.size - 1 - degree
        updated = np.zeros((points.size, columns))
        for i in range(columns):
            lower_gap = knot_row[i + degree] - knot_row[i]
            upper_gap = knot_row[i + degree + 1] - knot_row[i + 1]
            if lower_gap > 0:
                updated[:, i] += (points - knot_row[i]) / lower_gap * current[:, i]
            if upper_gap > 0:
                updated[:, i] += (knot_row[i + degree + 1] - points) / upper_gap * current[:, i + 1]
        previous = current
        current = updated
    slopes = np.zeros(current.shape)
    for i in range(current.shape[1]):
        lower_gap = knot_row[i + 3] - knot_row[i]
        upper_gap = knot_row[i + 4] - knot_row[i + 1]
        if lower_gap > 0:
            slopes[:, i] += 3.0 / lower_gap * previous[:, i]
        if upper_gap > 0:
            slopes[:, i] -= 3.0 / upper_gap * previous[:, i + 1]
    return (current.astype(np.float32), slopes.astype(np.float32))


def split(table):
    high = table.astype(np.float32).astype(BF16)
    low = (table.astype(np.float32) - high.astype(np.float32)).astype(BF16)
    return np.asarray(high), np.asarray(low)


def pair_table(first, second):
    wide_first = np.zeros((8, 8))
    wide_first[:, :7] = first
    wide_second = np.zeros((8, 8))
    wide_second[:, :7] = second
    return np.einsum("bj,ck->bcjk", wide_first, wide_second).reshape(64, 64)


def mirrored(table, flip_j, flip_k):
    grid = table.reshape(64, 8, 8).copy()
    if flip_j:
        grid[:, :7] = grid[:, 6::-1]
    if flip_k:
        grid[:, :, :7] = grid[:, :, 6::-1]
    return grid.reshape(64, 64)


def matmul_tables(values, slopes):
    value_value = pair_table(values, values)
    slope_value = pair_table(slopes, values)
    value_slope = pair_table(values, slopes)
    high, low = split(np.concatenate([value_value, slope_value, value_slope]))
    forward = np.concatenate([high, low, high], axis=1)
    back_mixed, back_plain = [], []
    for flips in range(4):
        vv, sv, vs = (
            split(mirrored(t, flips // 2, flips % 2).T) for t in (value_value, slope_value, value_slope)
        )
        none = np.zeros((64, 64), vv[0].dtype)
        mixed = np.concatenate([sv[0], vs[0]], axis=1)
        mixed_low = np.concatenate([sv[1], vs[1], none, none], axis=1)
        back_mixed.append(np.concatenate([np.concatenate([mixed, mixed], axis=1), mixed_low]))
        back_plain.append(
            np.concatenate(
                [
                    np.concatenate([vv[0], vv[0], none, none], axis=1),
                    np.concatenate([vv[1], none, none, none], axis=1),
                    np.concatenate([none, none, vv[0], vv[0]], axis=1),
                    np.concatenate([none, none, vv[1], none], axis=1),
                ]
            )
        )
    return forward, np.stack(back_mixed), np.stack(back_plain)


def halves(x):
    high = x.astype(BF16)
    low = (x - high.astype(F32)).astype(BF16)
    return high, low


def mac(terms):
    total = None
    for coefficient, x in terms:
        part = x * float(coefficient)
        total = part if total is None else total + part
    return total


def kernel(
    values, slopes, tiles,
    control, diag_in, off_in, weight_in, orient_in, forward_in, mixed_in_hbm, plain_in_hbm,
    stiff_out, mass_out,
    raw, orient, forward, mixed, plain,
    ubuf, gbuf, planes, metric, scales,
    xrecv, ysend_inner, yrecv_inner, ysend_ends, yrecv_ends, yrecv_sides,
    zsend_inner, zrecv_inner, zsend_sides, zrecv_sides,
    load_sem, small_sem, sems,
):
    px, py, pz = (lax.axis_index(a) for a in ("px", "py", "pz"))
    nx, ny, nz = (lax.axis_size(a) for a in ("px", "py", "pz"))
    x_up, x_down = lax.rem(px + 1, nx), lax.rem(px + nx - 1, nx)
    y_up, y_down = lax.rem(py + 1, ny), lax.rem(py + ny - 1, ny)
    z_up, z_down = lax.rem(pz + 1, nz), lax.rem(pz + nz - 1, nz)
    x_mirror = nx - 1 - px
    odd = lax.rem(px, 2)
    rim = 6 * odd

    def load(t):
        return pltpu.make_async_copy(
            control.at[:, :, :, pl.ds(pl.multiple_of(t * LANES, LANES), LANES)],
            ubuf.at[t, :, :, pl.ds(0, 7), :],
            load_sem.at[t],
        )

    small = [
        pltpu.make_async_copy(source, target, small_sem.at[n])
        for n, source, target in (
            (0, orient_in, orient),
            (1, diag_in, raw.at[pl.ds(0, 3)]),
            (1, off_in, raw.at[pl.ds(3, 3)]),
            (1, weight_in, raw.at[6]),
            (2, forward_in, forward),
            (3, mixed_in_hbm, mixed),
            (4, plain_in_hbm, plain),
        )
    ]
    load(0).start()
    for c in small:
        c.start()
    for t in range(1, tiles):
        load(t).start()

    barrier = pltpu.get_barrier_semaphore()
    for device in (
        (x_up, py, pz), (x_down, py, pz),
        (px, y_up, pz), (px, y_down, pz), (x_mirror, y_up, pz), (x_mirror, y_down, pz),
        (px, py, z_up), (px, py, z_down),
    ):
        pl.semaphore_signal(barrier, inc=1, device_id=device, device_id_type=MESH)

    pad = jnp.zeros((7, 7, 1, LANES), F32)
    for t in range(tiles):
        ubuf[t, :, :, pl.ds(7, 1), :] = pad

    small[0].wait()
    pltpu.make_async_copy(raw, raw, small_sem.at[1]).wait()
    flip_i, flip_j, flip_k = (orient[0, 0, 0, d] for d in range(3))
    variant = 2 * flip_j + flip_k

    scales[pl.ds(0, 56), pl.ds(0, 64)] = raw[...].reshape(56, 64)
    turned = scales[...].T[:64]

    def spread(m):
        metric[m] = jnp.broadcast_to(turned[:, m : m + 1], (64, LANES))

    def compute(t, first=False):
        load(t).wait()
        if first:
            for c in small[4:]:
                c.wait()
        forward_table = forward[...]
        mixed_table = mixed[variant]
        plain_table = plain[variant]
        nothing = jnp.zeros((8, LANES), F32)
        def ahead(e):
            source = [ubuf[t, i].reshape(56, LANES) for i in range(e, e + 4)]
            value_cat, slope_cat = [], []
            for a in (2 * e, 2 * e + 1):
                for table, cat in ((values, value_cat), (slopes, slope_cat)):
                    x = mac([(table[a, e + n], source[n]) for n in range(4)])
                    high, low = halves(jnp.concatenate([x, nothing], axis=0))
                    cat.append(jnp.concatenate([high, high, low], axis=0))
            at_values = jnp.dot(
                forward_table, jnp.concatenate(value_cat, axis=1), preferred_element_type=F32
            )
            at_slopes = jnp.dot(
                forward_table[:64], jnp.concatenate(slope_cat, axis=1), preferred_element_type=F32
            )
            return at_values, at_slopes

        def back(e, at_values, at_slopes):
            if first:
                for m in range(7):
                    spread(8 * m + 2 * e)
                    spread(8 * m + 2 * e + 1)
            mixed_in, plain_in = [], []
            for n, a in enumerate((2 * e, 2 * e + 1)):
                lanes = slice(n * LANES, (n + 1) * LANES)
                p, g2, g3 = (at_values[64 * r : 64 * r + 64, lanes] for r in range(3))
                g1 = at_slopes[:, lanes]
                d0, d1, d2, o0, o1, o2, w = (metric[8 * s + a] for s in range(7))
                f1 = d0 * g1 + o0 * g2 + o1 * g3
                f2 = o0 * g1 + d1 * g2 + o2 * g3
                f3 = o1 * g1 + o2 * g2 + d2 * g3
                f1h, f1l = halves(f1)
                f2h, f2l = halves(f2)
                f3h, f3l = halves(f3)
                mh, ml = halves(w * p)
                mixed_in.append(jnp.concatenate([f2h, f3h, f2l, f3l], axis=0))
                plain_in.append(jnp.concatenate([f1h, f1l, mh, ml], axis=0))
            mixed_back = jnp.dot(
                mixed_table, jnp.concatenate(mixed_in, axis=1), preferred_element_type=F32
            )
            plain_back = jnp.dot(
                plain_table, jnp.concatenate(plain_in, axis=1), preferred_element_type=F32
            )
            return mixed_back, plain_back

        def gather(e, mixed_back, plain_back):
            terms = []
            for n in range(2):
                lanes = slice(n * LANES, (n + 1) * LANES)
                terms.append(
                    (
                        plain_back[0:56, lanes] + plain_back[64:120, lanes],
                        mixed_back[0:56, lanes] + mixed_back[64:120, lanes],
                        plain_back[128:184, lanes] + plain_back[192:248, lanes],
                    )
                )
            for i in range(e, e + 4):
                stiff = mac(
                    [(slopes[2 * e + n, i], terms[n][0]) for n in range(2)]
                    + [(values[2 * e + n, i], terms[n][1]) for n in range(2)]
                )
                mass = mac([(values[2 * e + n, i], terms[n][2]) for n in range(2)])
                if e > 0 and i < e + 3:
                    stiff = stiff + planes[0, i]
                    mass = mass + planes[1, i]
                planes[0, i] = stiff
                planes[1, i] = mass

        up = {0: ahead(0), 1: ahead(1)}
        down = {}
        for e in range(4):
            down[e] = back(e, *up.pop(e))
            if e + 2 < 4:
                up[e + 2] = ahead(e + 2)
            if e >= 1:
                gather(e - 1, *down.pop(e - 1))
        gather(3, *down.pop(3))
        for o in range(2):
            for i in range(7):
                gbuf[o, t, i] = planes[o, i + flip_i * (6 - 2 * i)].reshape(7, 8, LANES)

    def remote(t, which, src, dst, device):
        return pltpu.make_async_remote_copy(
            src_ref=src, dst_ref=dst, send_sem=sems.at[t, which], recv_sem=sems.at[t, which],
            device_id=device, device_id_type=MESH,
        )

    rows = pl.ds(0, 7)

    def x_copies(t):
        return [
            remote(t, 0, gbuf.at[:, t, 6, :, rows, :], xrecv.at[t, 0, :, :, rows, :], (x_up, py, pz)),
            remote(t, 0, gbuf.at[:, t, 0, :, rows, :], xrecv.at[t, 1, :, :, rows, :], (x_down, py, pz)),
        ]

    def y_pair(t, which, sent, received):
        return [
            remote(t, which, sent.at[t, 1], received.at[t, 0], (px, y_up, pz)),
            remote(t, which, sent.at[t, 0], received.at[t, 1], (px, y_down, pz)),
        ]

    def y_inner(t):
        return y_pair(t, 1, ysend_inner, yrecv_inner)

    def y_ends(t):
        return y_pair(t, 2, ysend_ends, yrecv_ends)

    def y_sides(t):
        near = 6 - rim
        there = 1 - odd
        return [
            remote(t, 3, gbuf.at[:, t, near, 6, rows, :], yrecv_sides.at[t, 0, there, :, rows, :], (px, y_up, pz)),
            remote(t, 3, gbuf.at[:, t, near, 0, rows, :], yrecv_sides.at[t, 1, there, :, rows, :], (px, y_down, pz)),
            remote(t, 3, gbuf.at[:, t, rim, 6, rows, :], yrecv_sides.at[t, 0, there, :, rows, :], (x_mirror, y_up, pz)),
            remote(t, 3, gbuf.at[:, t, rim, 0, rows, :], yrecv_sides.at[t, 1, there, :, rows, :], (x_mirror, y_down, pz)),
        ]

    def z_pair(t, which, sent, received):
        return [
            remote(t, which, sent.at[t, 1], received.at[t, 0], (px, py, z_up)),
            remote(t, which, sent.at[t, 0], received.at[t, 1], (px, py, z_down)),
        ]

    def z_inner(t):
        return z_pair(t, 4, zsend_inner, zrecv_inner)

    def z_sides(t):
        return z_pair(t, 5, zsend_sides, zrecv_sides)

    def start(copies):
        for c in copies:
            c.start()

    def wait(t, which):
        views = (
            xrecv.at[pl.ds(0, 2), :, :, :, rows, :],
            yrecv_inner.at[pl.ds(0, 2)],
            yrecv_ends.at[pl.ds(0, 2)],
            yrecv_sides.at[pl.ds(0, 2), :, :, :, rows, :],
            zrecv_inner.at[pl.ds(0, 2)],
            zrecv_sides.at[pl.ds(0, 2)],
        )
        pltpu.make_async_copy(views[which], views[which], sems.at[t, which]).wait()

    def fold_x(t):
        for side in range(2):
            for o in range(2):
                gbuf[o, t, 6 * side, :, rows, :] = (
                    gbuf[o, t, 6 * side, :, rows, :] + xrecv[t, side, o, :, rows, :]
                )

    inner_rows = [(i, i - 1) for i in range(1, 6)]
    side_rows = [(6 * n, n) for n in range(2)]

    def take_z(t, sent, where):
        for side in range(2):
            for o in range(2):
                for i, n in where:
                    sent[t, side, o, n] = gbuf[o, t, i, :, 6 * side, :]

    def fold_z(t, received, where):
        for side in range(2):
            for o in range(2):
                for i, n in where:
                    gbuf[o, t, i, :, 6 * side, :] = gbuf[o, t, i, :, 6 * side, :] + received[t, side, o, n]

    mid = pl.ds(1, 5)

    def take_y_inner(t):
        for side in range(2):
            for o in range(2):
                ysend_inner[t, side, o] = gbuf[o, t, mid, 6 * side, mid, :]

    def take_y_ends(t):
        for side in range(2):
            for o in range(2):
                for n in range(2):
                    ysend_ends[t, side, o, n] = gbuf[o, t, mid, 6 * side, 6 * n, :]

    def fold_y(t):
        for side in range(2):
            for o in range(2):
                j = 6 * side
                gbuf[o, t, mid, j, mid, :] = gbuf[o, t, mid, j, mid, :] + yrecv_inner[t, side, o]
                for n in range(2):
                    gbuf[o, t, mid, j, 6 * n, :] = gbuf[o, t, mid, j, 6 * n, :] + yrecv_ends[t, side, o, n]
                    gbuf[o, t, 6 * n, j, rows, :] = gbuf[o, t, 6 * n, j, rows, :] + yrecv_sides[t, side, n, o, rows, :]

    sublane = lax.broadcasted_iota(jnp.int32, (8, LANES), 0)
    turned_rows = jnp.where(sublane < 7, 6 - sublane, sublane)
    pick = sublane + flip_k * (turned_rows - sublane)

    def finish(t):
        lanes = pl.ds(pl.multiple_of(t * LANES, LANES), LANES)
        for o, out in enumerate((stiff_out, mass_out)):
            for i in range(7):
                for j in range(7):
                    tile = gbuf[o, t, i + flip_i * (6 - 2 * i), j + flip_j * (6 - 2 * j)]
                    out[i, j, :, lanes] = jnp.take_along_axis(tile, pick, axis=0)[:7]

    def send_first(t):
        start(x_copies(t))
        take_z(t, zsend_inner, inner_rows)
        start(z_inner(t))
        take_y_inner(t)

    def produce(t, carry):
        compute(t)
        send_first(t)
        start(y_inner(t - 1))
        return carry

    def after_x(t, carry):
        wait(t, 0)
        fold_x(t)
        take_z(t, zsend_sides, side_rows)
        start(z_sides(t))
        return carry

    def after_z(t, carry):
        wait(t, 4)
        fold_z(t, zrecv_inner, inner_rows)
        take_y_ends(t)
        start(y_ends(t))
        wait(t, 5)
        fold_z(t, zrecv_sides, side_rows)
        start(y_sides(t))
        return carry

    def after_y(t, carry):
        wait(t, 1)
        wait(t, 2)
        wait(t, 3)
        fold_y(t)
        finish(t)
        return carry

    compute(0, first=True)
    pl.semaphore_wait(barrier, 8)
    send_first(0)
    lax.fori_loop(1, tiles, produce, 0)
    start(y_inner(tiles - 1))
    for stage in (after_x, after_z, after_y):
        lax.fori_loop(0, tiles, stage, 0)


def put(stiff, mass, stiff_out, mass_out, sem):
    copies = [
        pltpu.make_async_copy(source, target, sem.at[n])
        for n, (source, target) in enumerate(((stiff, stiff_out), (mass, mass_out)))
    ]
    for c in copies:
        c.start()
    for c in copies:
        c.wait()


def per_device(control_values, metric_diag, metric_off, mass_weight, orient):
    values, slopes = spline_tables(4)
    tiles = control_values.shape[-1] // LANES
    forward, mixed, plain = (jnp.asarray(t) for t in matmul_tables(values, slopes))
    shape = jax.ShapeDtypeStruct(control_values.shape, F32)
    in_vmem = pl.BlockSpec(memory_space=pltpu.VMEM)
    in_hbm = pl.BlockSpec(memory_space=pltpu.HBM)
    results = pl.pallas_call(
        functools.partial(kernel, values, slopes, tiles),
        out_shape=(pltpu.VMEM(control_values.shape, F32),) * 2,
        in_specs=[in_hbm] * 8,
        out_specs=(in_vmem, in_vmem),
        scratch_shapes=[
            pltpu.VMEM((7, 8, 64), F32),
            pltpu.SMEM(orient.shape, jnp.int32),
            pltpu.VMEM(forward.shape, BF16),
            pltpu.VMEM(mixed.shape, BF16),
            pltpu.VMEM(plain.shape, BF16),
            pltpu.VMEM((tiles, 7, 7, 8, LANES), F32),
            pltpu.VMEM((2, tiles, 7, 7, 8, LANES), F32),
            pltpu.VMEM((2, 7, 56, LANES), F32),
            pltpu.VMEM((56, 64, LANES), F32),
            pltpu.VMEM((128, 128), F32),
            pltpu.VMEM((tiles, 2, 2, 7, 8, LANES), F32),
            pltpu.VMEM((tiles, 2, 2, 5, 5, LANES), F32),
            pltpu.VMEM((tiles, 2, 2, 5, 5, LANES), F32),
            pltpu.VMEM((tiles, 2, 2, 2, 5, LANES), F32),
            pltpu.VMEM((tiles, 2, 2, 2, 5, LANES), F32),
            pltpu.VMEM((tiles, 2, 2, 2, 8, LANES), F32),
            pltpu.VMEM((tiles, 2, 2, 5, 7, LANES), F32),
            pltpu.VMEM((tiles, 2, 2, 5, 7, LANES), F32),
            pltpu.VMEM((tiles, 2, 2, 2, 7, LANES), F32),
            pltpu.VMEM((tiles, 2, 2, 2, 7, LANES), F32),
            pltpu.SemaphoreType.DMA((tiles,)),
            pltpu.SemaphoreType.DMA((5,)),
            pltpu.SemaphoreType.DMA((tiles, 6)),
        ],
        compiler_params=pltpu.CompilerParams(
            collective_id=0, has_side_effects=True, vmem_limit_bytes=40 * 1024 * 1024
        ),
        name="apply",
    )(
        *(
            pltpu.with_memory_space_constraint(x, pltpu.HBM)
            for x in (control_values, metric_diag, metric_off, mass_weight, orient, forward, mixed, plain)
        )
    )
    return pl.pallas_call(
        put,
        out_shape=(shape, shape),
        in_specs=[pl.BlockSpec(memory_space=pl.ANY)] * 2,
        out_specs=(in_hbm, in_hbm),
        scratch_shapes=[pltpu.SemaphoreType.DMA((2,))],
        compiler_params=pltpu.CompilerParams(vmem_limit_bytes=1024 * 1024),
        name="put",
    )(*(pltpu.with_memory_space_constraint(x, pltpu.VMEM) for x in results))


def solution(mesh):
    in_specs = (
        P("px", "py", "pz", None),
        P(None, "px", ("py", "pz")),
        P(None, "px", ("py", "pz")),
        P("px", ("py", "pz")),
        P("px", "py", "pz", None),
    )
    out_specs = (P("px", "py", "pz", None), P("px", "py", "pz", None))
    return jax.shard_map(
        per_device, mesh=mesh, in_specs=in_specs, out_specs=out_specs, check_vma=False
    )
```

```python
import functools
import math

import jax
import jax.numpy as jnp
import numpy as np
from jax import lax
from jax.experimental import pallas as pl
from jax.experimental.pallas import tpu as pltpu
from jax.sharding import PartitionSpec as P

MESH = pl.DeviceIdType.MESH
LANES = 128
LAG = 2
F32 = jnp.float32
BF16 = jnp.bfloat16


def spline_tables(elements):
    knot_row = np.concatenate(
        [np.zeros(3), np.arange(elements + 1) * 1.0, np.full(3, float(elements))]
    )
    offsets = np.array([0.5 - 0.5 / math.sqrt(3.0), 0.5 + 0.5 / math.sqrt(3.0)])
    points = (np.arange(elements)[:, None] + offsets[None, :]).reshape(-1)
    intervals = np.repeat(np.arange(elements), 2) + 3
    current = np.zeros((points.size, knot_row.size - 1))
    current[np.arange(points.size), intervals] = 1.0
    previous = current
    for degree in range(1, 4):
        columns = knot_row.size - 1 - degree
        updated = np.zeros((points.size, columns))
        for i in range(columns):
            lower_gap = knot_row[i + degree] - knot_row[i]
            upper_gap = knot_row[i + degree + 1] - knot_row[i + 1]
            if lower_gap > 0:
                updated[:, i] += (points - knot_row[i]) / lower_gap * current[:, i]
            if upper_gap > 0:
                updated[:, i] += (knot_row[i + degree + 1] - points) / upper_gap * current[:, i + 1]
        previous = current
        current = updated
    slopes = np.zeros(current.shape)
    for i in range(current.shape[1]):
        lower_gap = knot_row[i + 3] - knot_row[i]
        upper_gap = knot_row[i + 4] - knot_row[i + 1]
        if lower_gap > 0:
            slopes[:, i] += 3.0 / lower_gap * previous[:, i]
        if upper_gap > 0:
            slopes[:, i] -= 3.0 / upper_gap * previous[:, i + 1]
    return (current.astype(np.float32), slopes.astype(np.float32))


def split(table):
    high = table.astype(np.float32).astype(BF16)
    low = (table.astype(np.float32) - high.astype(np.float32)).astype(BF16)
    return np.asarray(high), np.asarray(low)


def pair_table(first, second):
    wide_first = np.zeros((8, 8))
    wide_first[:, :7] = first
    wide_second = np.zeros((8, 8))
    wide_second[:, :7] = second
    return np.einsum("bj,ck->bcjk", wide_first, wide_second).reshape(64, 64)


def mirrored(table, flip_k):
    grid = table.reshape(64, 8, 8).copy()
    if flip_k:
        grid[:, :, :7] = grid[:, :, 6::-1]
    return grid.reshape(64, 64)


def matmul_tables(values, slopes):
    value_value = pair_table(values, values)
    slope_value = pair_table(slopes, values)
    value_slope = pair_table(values, slopes)
    high, low = split(np.concatenate([value_value, slope_value, value_slope]))
    forward = np.concatenate([high, low, high], axis=1)
    back_mixed, back_plain = [], []
    for flip_k in range(2):
        vv, sv, vs = (
            split(mirrored(t, flip_k).T) for t in (value_value, slope_value, value_slope)
        )
        none = np.zeros((64, 64), vv[0].dtype)
        mixed = np.concatenate([sv[0], vs[0]], axis=1)
        mixed_low = np.concatenate([sv[1], vs[1], none, none], axis=1)
        back_mixed.append(np.concatenate([np.concatenate([mixed, mixed], axis=1), mixed_low]))
        back_plain.append(
            np.concatenate(
                [
                    np.concatenate([vv[0], vv[0], none, none], axis=1),
                    np.concatenate([vv[1], none, none, none], axis=1),
                    np.concatenate([none, none, vv[0], vv[0]], axis=1),
                    np.concatenate([none, none, vv[1], none], axis=1),
                ]
            )
        )
    return forward, np.stack(back_mixed), np.stack(back_plain)


def halves(x):
    high = x.astype(BF16)
    low = (x - high.astype(F32)).astype(BF16)
    return high, low


def mac(terms):
    total = None
    for coefficient, x in terms:
        part = x * float(coefficient)
        total = part if total is None else total + part
    return total


def kernel(
    values, slopes, tiles,
    control, diag_in, off_in, weight_in, orient_in, forward_in, mixed_in_hbm, plain_in_hbm,
    stiff_out, mass_out,
    raw, orient, forward, mixed, plain,
    ubuf, gbuf, planes, metric, scales,
    xrecv, ysend_inner, yrecv_inner, ysend_ends, yrecv_ends,
    ysend_sides, yrecv_sides, ysend_corners, yrecv_corners,
    zsend_inner, zrecv_inner, zsend_sides, zrecv_sides,
    load_sem, small_sem, sems,
):
    px, py, pz = (lax.axis_index(a) for a in ("px", "py", "pz"))
    nx, ny, nz = (lax.axis_size(a) for a in ("px", "py", "pz"))
    x_up, x_down = lax.rem(px + 1, nx), lax.rem(px + nx - 1, nx)
    y_up, y_down = lax.rem(py + 1, ny), lax.rem(py + ny - 1, ny)
    z_up, z_down = lax.rem(pz + 1, nz), lax.rem(pz + nz - 1, nz)
    x_mirror = nx - 1 - px
    odd = lax.rem(px, 2)

    barrier = pltpu.get_barrier_semaphore()
    for device in (
        (x_up, py, pz), (x_down, py, pz),
        (px, y_up, pz), (px, y_down, pz), (x_mirror, y_up, pz), (x_mirror, y_down, pz),
        (px, py, z_up), (px, py, z_down),
    ):
        pl.semaphore_signal(barrier, inc=1, device_id=device, device_id_type=MESH)

    def load(t):
        return pltpu.make_async_copy(
            control.at[:, :, :, pl.ds(pl.multiple_of(t * LANES, LANES), LANES)],
            ubuf.at[t, :, :, pl.ds(0, 7), :],
            load_sem.at[t],
        )

    small = [
        pltpu.make_async_copy(source, target, small_sem.at[n])
        for n, source, target in (
            (0, orient_in, orient),
            (1, diag_in, raw.at[pl.ds(0, 3)]),
            (1, off_in, raw.at[pl.ds(3, 3)]),
            (1, weight_in, raw.at[6]),
            (2, forward_in, forward),
            (3, mixed_in_hbm, mixed),
            (4, plain_in_hbm, plain),
        )
    ]
    load(0).start()
    for c in small:
        c.start()
    for t in range(1, tiles):
        load(t).start()

    pad = jnp.zeros((7, 7, 1, LANES), F32)
    for t in range(tiles):
        ubuf[t, :, :, pl.ds(7, 1), :] = pad

    small[0].wait()
    pltpu.make_async_copy(raw, raw, small_sem.at[1]).wait()
    flip_i, flip_j, flip_k = (orient[0, 0, 0, d] for d in range(3))

    scales[pl.ds(0, 56), pl.ds(0, 64)] = raw[...].reshape(56, 64)
    turned = scales[...].T[:64]

    def spread(m):
        metric[m] = jnp.broadcast_to(turned[:, m : m + 1], (64, LANES))

    def compute(t, first=False):
        load(t).wait()
        if first:
            small[4].wait()
        forward_table = forward[...]
        nothing = jnp.zeros((8, LANES), F32)
        def ahead(e):
            source = [ubuf[t, i].reshape(56, LANES) for i in range(e, e + 4)]
            value_cat, slope_cat = [], []
            for a in (2 * e, 2 * e + 1):
                for table, cat in ((values, value_cat), (slopes, slope_cat)):
                    x = mac([(table[a, e + n], source[n]) for n in range(4)])
                    high, low = halves(jnp.concatenate([x, nothing], axis=0))
                    cat.append(jnp.concatenate([high, high, low], axis=0))
            at_values = jnp.dot(
                forward_table, jnp.concatenate(value_cat, axis=1), preferred_element_type=F32
            )
            at_slopes = jnp.dot(
                forward_table[:64], jnp.concatenate(slope_cat, axis=1), preferred_element_type=F32
            )
            return at_values, at_slopes

        def back(e, at_values, at_slopes):
            if first:
                for m in range(7):
                    spread(8 * m + 2 * e)
                    spread(8 * m + 2 * e + 1)
            mixed_in, plain_in = [], []
            for n, a in enumerate((2 * e, 2 * e + 1)):
                lanes = slice(n * LANES, (n + 1) * LANES)
                p, g2, g3 = (at_values[64 * r : 64 * r + 64, lanes] for r in range(3))
                g1 = at_slopes[:, lanes]
                d0, d1, d2, o0, o1, o2, w = (metric[8 * s + a] for s in range(7))
                f1 = d0 * g1 + o0 * g2 + o1 * g3
                f2 = o0 * g1 + d1 * g2 + o2 * g3
                f3 = o1 * g1 + o2 * g2 + d2 * g3
                f1h, f1l = halves(f1)
                f2h, f2l = halves(f2)
                f3h, f3l = halves(f3)
                mh, ml = halves(w * p)
                mixed_in.append(jnp.concatenate([f2h, f3h, f2l, f3l], axis=0))
                plain_in.append(jnp.concatenate([f1h, f1l, mh, ml], axis=0))
            mixed_back = jnp.dot(
                mixed_table, jnp.concatenate(mixed_in, axis=1), preferred_element_type=F32
            )
            plain_back = jnp.dot(
                plain_table, jnp.concatenate(plain_in, axis=1), preferred_element_type=F32
            )
            return mixed_back, plain_back

        def gather(e, mixed_back, plain_back):
            terms = []
            for n in range(2):
                lanes = slice(n * LANES, (n + 1) * LANES)
                terms.append(
                    (
                        plain_back[0:56, lanes] + plain_back[64:120, lanes],
                        mixed_back[0:56, lanes] + mixed_back[64:120, lanes],
                        plain_back[128:184, lanes] + plain_back[192:248, lanes],
                    )
                )
            for i in range(e, e + 4):
                stiff = mac(
                    [(slopes[2 * e + n, i], terms[n][0]) for n in range(2)]
                    + [(values[2 * e + n, i], terms[n][1]) for n in range(2)]
                )
                mass = mac([(values[2 * e + n, i], terms[n][2]) for n in range(2)])
                if e > 0 and i < e + 3:
                    stiff = stiff + planes[0, i].reshape(56, LANES)
                    mass = mass + planes[1, i].reshape(56, LANES)
                planes[0, i] = stiff.reshape(7, 8, LANES)
                planes[1, i] = mass.reshape(7, 8, LANES)

        up = {e: ahead(e) for e in range(4)}
        if first:
            small[5].wait()
            small[6].wait()
        mixed_table = mixed[flip_k]
        plain_table = plain[flip_k]
        down = {}
        for e in range(4):
            down[e] = back(e, *up.pop(e))
            if e >= 1:
                gather(e - 1, *down.pop(e - 1))
        for e in range(4 - 1, 4):
            gather(e, *down.pop(e))
        for o in range(2):
            for i in range(7):
                for j in range(7):
                    gbuf[o, t, i, j] = planes[o, i + flip_i * (6 - 2 * i), j + flip_j * (6 - 2 * j)]

    def remote(t, which, src, dst, device):
        return pltpu.make_async_remote_copy(
            src_ref=src, dst_ref=dst, send_sem=sems.at[t, which], recv_sem=sems.at[t, which],
            device_id=device, device_id_type=MESH,
        )

    rows = pl.ds(0, 7)

    def x_copies(t):
        return [
            remote(t, 0, gbuf.at[:, t, 6, :, rows, :], xrecv.at[t, 0, :, :, rows, :], (x_up, py, pz)),
            remote(t, 0, gbuf.at[:, t, 0, :, rows, :], xrecv.at[t, 1, :, :, rows, :], (x_down, py, pz)),
        ]

    def y_pair(t, which, sent, received):
        return [
            remote(t, which, sent.at[t, 1], received.at[t, 0], (px, y_up, pz)),
            remote(t, which, sent.at[t, 0], received.at[t, 1], (px, y_down, pz)),
        ]

    def y_inner(t):
        return y_pair(t, 1, ysend_inner, yrecv_inner)

    def y_ends(t):
        return y_pair(t, 2, ysend_ends, yrecv_ends)

    def y_rims(t, which, sent, received):
        near = 1 - odd
        return [
            remote(t, which, sent.at[t, 1, near], received.at[t, 0, near], (px, y_up, pz)),
            remote(t, which, sent.at[t, 0, near], received.at[t, 1, near], (px, y_down, pz)),
            remote(t, which, sent.at[t, 1, odd], received.at[t, 0, near], (x_mirror, y_up, pz)),
            remote(t, which, sent.at[t, 0, odd], received.at[t, 1, near], (x_mirror, y_down, pz)),
        ]

    def y_sides(t):
        return y_rims(t, 3, ysend_sides, yrecv_sides)

    def y_corners(t):
        return y_rims(t, 6, ysend_corners, yrecv_corners)

    def z_pair(t, which, sent, received):
        return [
            remote(t, which, sent.at[t, 1], received.at[t, 0], (px, py, z_up)),
            remote(t, which, sent.at[t, 0], received.at[t, 1], (px, py, z_down)),
        ]

    def z_inner(t):
        return z_pair(t, 4, zsend_inner, zrecv_inner)

    def z_sides(t):
        return z_pair(t, 5, zsend_sides, zrecv_sides)

    def start(copies):
        for c in copies:
            c.start()

    def wait(t, which):
        views = (
            xrecv.at[pl.ds(0, 2), :, :, :, rows, :],
            yrecv_inner.at[pl.ds(0, 2)],
            yrecv_ends.at[pl.ds(0, 2)],
            yrecv_sides.at[pl.ds(0, 2)],
            zrecv_inner.at[pl.ds(0, 2)],
            zrecv_sides.at[pl.ds(0, 2)],
            yrecv_corners.at[pl.ds(0, 2)],
        )
        pltpu.make_async_copy(views[which], views[which], sems.at[t, which]).wait()

    def fold_x(t):
        for side in range(2):
            for o in range(2):
                gbuf[o, t, 6 * side, :, rows, :] = (
                    gbuf[o, t, 6 * side, :, rows, :] + xrecv[t, side, o, :, rows, :]
                )

    inner_rows = [(i, i - 1) for i in range(1, 6)]
    side_rows = [(6 * n, n) for n in range(2)]

    def take_z(t, sent, where):
        for side in range(2):
            for o in range(2):
                for i, n in where:
                    sent[t, side, o, n] = gbuf[o, t, i, :, 6 * side, :]

    def fold_z(t, received, where):
        for side in range(2):
            for o in range(2):
                for i, n in where:
                    gbuf[o, t, i, :, 6 * side, :] = gbuf[o, t, i, :, 6 * side, :] + received[t, side, o, n]

    mid = pl.ds(1, 5)

    def take_y_inner(t):
        for side in range(2):
            for o in range(2):
                ysend_inner[t, side, o] = gbuf[o, t, mid, 6 * side, mid, :]

    def take_y_ends(t):
        for side in range(2):
            for o in range(2):
                for n in range(2):
                    ysend_ends[t, side, o, n] = gbuf[o, t, mid, 6 * side, 6 * n, :]

    def take_y_sides(t):
        for side in range(2):
            for o in range(2):
                for n in range(2):
                    ysend_sides[t, side, n, o] = gbuf[o, t, 6 * n, 6 * side, mid, :]

    def take_y_corners(t):
        for side in range(2):
            for o in range(2):
                for n in range(2):
                    for m in range(2):
                        ysend_corners[t, side, n, o, m] = gbuf[o, t, 6 * n, 6 * side, 6 * m, :]

    def fold_y(t):
        for side in range(2):
            for o in range(2):
                j = 6 * side
                gbuf[o, t, mid, j, mid, :] = gbuf[o, t, mid, j, mid, :] + yrecv_inner[t, side, o]
                for n in range(2):
                    gbuf[o, t, mid, j, 6 * n, :] = gbuf[o, t, mid, j, 6 * n, :] + yrecv_ends[t, side, o, n]
                    gbuf[o, t, 6 * n, j, mid, :] = gbuf[o, t, 6 * n, j, mid, :] + yrecv_sides[t, side, n, o]

    def fold_corners(t):
        for side in range(2):
            for o in range(2):
                for n in range(2):
                    for m in range(2):
                        gbuf[o, t, 6 * n, 6 * side, 6 * m, :] = (
                            gbuf[o, t, 6 * n, 6 * side, 6 * m, :] + yrecv_corners[t, side, n, o, m]
                        )

    sublane = lax.broadcasted_iota(jnp.int32, (8, LANES), 0)
    turned_rows = jnp.where(sublane < 7, 6 - sublane, sublane)
    pick = sublane + flip_k * (turned_rows - sublane)

    def finish(t, where):
        lanes = pl.ds(pl.multiple_of(t * LANES, LANES), LANES)
        for o, out in enumerate((stiff_out, mass_out)):
            for i, j in where:
                tile = gbuf[o, t, i + flip_i * (6 - 2 * i), j + flip_j * (6 - 2 * j)]
                out[i, j, :, lanes] = jnp.take_along_axis(tile, pick, axis=0)[:7]

    def send_first(t):
        start(x_copies(t))
        take_z(t, zsend_inner, inner_rows)
        start(z_inner(t))
        take_y_inner(t)

    def produce(t, carry):
        compute(t)
        send_first(t)
        start(y_inner(t - 1))
        return carry

    def after_x(t):
        wait(t, 4)
        fold_z(t, zrecv_inner, inner_rows)
        take_y_ends(t)
        start(y_ends(t))
        wait(t, 0)
        fold_x(t)
        take_z(t, zsend_sides, side_rows)
        start(z_sides(t))
        take_y_sides(t)
        start(y_sides(t))

    def after_z(t):
        wait(t, 5)
        fold_z(t, zrecv_sides, side_rows)
        take_y_corners(t)
        start(y_corners(t))

    def exchange(t, carry):
        after_x(t)

        @pl.when(t >= LAG)
        def _():
            after_z(t - LAG)

        return carry

    def rest(t, carry):
        after_z(t)
        return carry

    between = [(i, j) for i in range(7) for j in range(1, 6)]
    faces = [(i, j) for i in range(1, 6) for j in (0, 6)]
    corners = [(i, j) for i in (0, 6) for j in (0, 6)]

    def close(t, carry):
        finish(t, between)
        return carry

    def after_y(t, carry):
        for which in (1, 2, 3):
            wait(t, which)
        fold_y(t)
        finish(t, faces)
        return carry

    def after_corners(t, carry):
        wait(t, 6)
        fold_corners(t)
        finish(t, corners)
        return carry

    compute(0, first=True)
    pl.semaphore_wait(barrier, 8)
    send_first(0)
    lax.fori_loop(1, tiles, produce, 0)
    start(y_inner(tiles - 1))
    lax.fori_loop(0, tiles, exchange, 0)
    lax.fori_loop(tiles - LAG, tiles, rest, 0)
    for stage in (close, after_y, after_corners):
        lax.fori_loop(0, tiles, stage, 0)


def put(stiff, mass, stiff_out, mass_out, sem):
    copies = [
        pltpu.make_async_copy(source, target, sem.at[n])
        for n, (source, target) in enumerate(((stiff, stiff_out), (mass, mass_out)))
    ]
    for c in copies:
        c.start()
    for c in copies:
        c.wait()


def per_device(control_values, metric_diag, metric_off, mass_weight, orient):
    values, slopes = spline_tables(4)
    tiles = control_values.shape[-1] // LANES
    forward, mixed, plain = (jnp.asarray(t) for t in matmul_tables(values, slopes))
    shape = jax.ShapeDtypeStruct(control_values.shape, F32)
    in_vmem = pl.BlockSpec(memory_space=pltpu.VMEM)
    in_hbm = pl.BlockSpec(memory_space=pltpu.HBM)
    results = pl.pallas_call(
        functools.partial(kernel, values, slopes, tiles),
        out_shape=(pltpu.VMEM(control_values.shape, F32),) * 2,
        in_specs=[in_hbm] * 8,
        out_specs=(in_vmem, in_vmem),
        scratch_shapes=[
            pltpu.VMEM((7, 8, 64), F32),
            pltpu.SMEM(orient.shape, jnp.int32),
            pltpu.VMEM(forward.shape, BF16),
            pltpu.VMEM(mixed.shape, BF16),
            pltpu.VMEM(plain.shape, BF16),
            pltpu.VMEM((tiles, 7, 7, 8, LANES), F32),
            pltpu.VMEM((2, tiles, 7, 7, 8, LANES), F32),
            pltpu.VMEM((2, 7, 7, 8, LANES), F32),
            pltpu.VMEM((56, 64, LANES), F32),
            pltpu.VMEM((128, 128), F32),
            pltpu.VMEM((tiles, 2, 2, 7, 8, LANES), F32),
            pltpu.VMEM((tiles, 2, 2, 5, 5, LANES), F32),
            pltpu.VMEM((tiles, 2, 2, 5, 5, LANES), F32),
            pltpu.VMEM((tiles, 2, 2, 2, 5, LANES), F32),
            pltpu.VMEM((tiles, 2, 2, 2, 5, LANES), F32),
            pltpu.VMEM((tiles, 2, 2, 2, 5, LANES), F32),
            pltpu.VMEM((tiles, 2, 2, 2, 5, LANES), F32),
            pltpu.VMEM((tiles, 2, 2, 2, 2, LANES), F32),
            pltpu.VMEM((tiles, 2, 2, 2, 2, LANES), F32),
            pltpu.VMEM((tiles, 2, 2, 5, 7, LANES), F32),
            pltpu.VMEM((tiles, 2, 2, 5, 7, LANES), F32),
            pltpu.VMEM((tiles, 2, 2, 2, 7, LANES), F32),
            pltpu.VMEM((tiles, 2, 2, 2, 7, LANES), F32),
            pltpu.SemaphoreType.DMA((tiles,)),
            pltpu.SemaphoreType.DMA((5,)),
            pltpu.SemaphoreType.DMA((tiles, 7)),
        ],
        compiler_params=pltpu.CompilerParams(
            collective_id=0, has_side_effects=True, vmem_limit_bytes=40 * 1024 * 1024
        ),
        name="apply",
    )(
        *(
            pltpu.with_memory_space_constraint(x, pltpu.HBM)
            for x in (control_values, metric_diag, metric_off, mass_weight, orient, forward, mixed, plain)
        )
    )
    return pl.pallas_call(
        put,
        out_shape=(shape, shape),
        in_specs=[pl.BlockSpec(memory_space=pl.ANY)] * 2,
        out_specs=(in_hbm, in_hbm),
        scratch_shapes=[pltpu.SemaphoreType.DMA((2,))],
        compiler_params=pltpu.CompilerParams(vmem_limit_bytes=1024 * 1024),
        name="put",
    )(*(pltpu.with_memory_space_constraint(x, pltpu.VMEM) for x in results))


def solution(mesh):
    in_specs = (
        P("px", "py", "pz", None),
        P(None, "px", ("py", "pz")),
        P(None, "px", ("py", "pz")),
        P("px", ("py", "pz")),
        P("px", "py", "pz", None),
    )
    out_specs = (P("px", "py", "pz", None), P("px", "py", "pz", None))
    return jax.shard_map(
        per_device, mesh=mesh, in_specs=in_specs, out_specs=out_specs, check_vma=False
    )
```

```python
import functools
import math

import jax
import jax.numpy as jnp
import numpy as np
from jax import lax
from jax.experimental import pallas as pl
from jax.experimental.pallas import tpu as pltpu
from jax.sharding import PartitionSpec as P

MESH = pl.DeviceIdType.MESH
LANES = 128
F32 = jnp.float32
BF16 = jnp.bfloat16


def spline_tables(elements):
    knot_row = np.concatenate(
        [np.zeros(3), np.arange(elements + 1) * 1.0, np.full(3, float(elements))]
    )
    offsets = np.array([0.5 - 0.5 / math.sqrt(3.0), 0.5 + 0.5 / math.sqrt(3.0)])
    points = (np.arange(elements)[:, None] + offsets[None, :]).reshape(-1)
    intervals = np.repeat(np.arange(elements), 2) + 3
    current = np.zeros((points.size, knot_row.size - 1))
    current[np.arange(points.size), intervals] = 1.0
    previous = current
    for degree in range(1, 4):
        columns = knot_row.size - 1 - degree
        updated = np.zeros((points.size, columns))
        for i in range(columns):
            lower_gap = knot_row[i + degree] - knot_row[i]
            upper_gap = knot_row[i + degree + 1] - knot_row[i + 1]
            if lower_gap > 0:
                updated[:, i] += (points - knot_row[i]) / lower_gap * current[:, i]
            if upper_gap > 0:
                updated[:, i] += (knot_row[i + degree + 1] - points) / upper_gap * current[:, i + 1]
        previous = current
        current = updated
    slopes = np.zeros(current.shape)
    for i in range(current.shape[1]):
        lower_gap = knot_row[i + 3] - knot_row[i]
        upper_gap = knot_row[i + 4] - knot_row[i + 1]
        if lower_gap > 0:
            slopes[:, i] += 3.0 / lower_gap * previous[:, i]
        if upper_gap > 0:
            slopes[:, i] -= 3.0 / upper_gap * previous[:, i + 1]
    return (current.astype(np.float32), slopes.astype(np.float32))


def split(table):
    high = table.astype(np.float32).astype(BF16)
    low = (table.astype(np.float32) - high.astype(np.float32)).astype(BF16)
    return np.asarray(high), np.asarray(low)


def pair_table(first, second):
    wide_first = np.zeros((8, 8))
    wide_first[:, :7] = first
    wide_second = np.zeros((8, 8))
    wide_second[:, :7] = second
    return np.einsum("bj,ck->bcjk", wide_first, wide_second).reshape(64, 64)


def mirrored(table, flip_j, flip_k):
    grid = table.reshape(64, 8, 8).copy()
    if flip_j:
        grid[:, :7] = grid[:, 6::-1]
    if flip_k:
        grid[:, :, :7] = grid[:, :, 6::-1]
    return grid.reshape(64, 64)


def matmul_tables(values, slopes):
    value_value = pair_table(values, values)
    slope_value = pair_table(slopes, values)
    value_slope = pair_table(values, slopes)
    high, low = split(np.concatenate([value_value, slope_value, value_slope]))
    forward = np.concatenate([high, low, high], axis=1)
    back_mixed, back_plain = [], []
    for flips in range(4):
        vv, sv, vs = (
            split(mirrored(t, flips // 2, flips % 2).T) for t in (value_value, slope_value, value_slope)
        )
        none = np.zeros((64, 64), vv[0].dtype)
        mixed = np.concatenate([sv[0], vs[0]], axis=1)
        mixed_low = np.concatenate([sv[1], vs[1], none, none], axis=1)
        back_mixed.append(np.concatenate([np.concatenate([mixed, mixed], axis=1), mixed_low]))
        back_plain.append(
            np.concatenate(
                [
                    np.concatenate([vv[0], vv[0], none, none], axis=1),
                    np.concatenate([vv[1], none, none, none], axis=1),
                    np.concatenate([none, none, vv[0], vv[0]], axis=1),
                    np.concatenate([none, none, vv[1], none], axis=1),
                ]
            )
        )
    return forward, np.stack(back_mixed), np.stack(back_plain)


def halves(x):
    high = x.astype(BF16)
    low = (x - high.astype(F32)).astype(BF16)
    return high, low


def mac(terms):
    total = None
    for coefficient, x in terms:
        part = x * float(coefficient)
        total = part if total is None else total + part
    return total


def kernel(
    values, slopes, tiles,
    control, diag_in, off_in, weight_in, orient_in, forward_in, mixed_in_hbm, plain_in_hbm,
    stiff_out, mass_out,
    raw, orient, forward, mixed, plain,
    ubuf, gbuf, planes, metric, scales,
    xrecv, ysend_inner, yrecv_inner, ysend_ends, yrecv_ends, yrecv_sides,
    zsend_inner, zrecv_inner, zsend_sides, zrecv_sides,
    load_sem, small_sem, sems,
):
    px, py, pz = (lax.axis_index(a) for a in ("px", "py", "pz"))
    nx, ny, nz = (lax.axis_size(a) for a in ("px", "py", "pz"))
    x_up, x_down = lax.rem(px + 1, nx), lax.rem(px + nx - 1, nx)
    y_up, y_down = lax.rem(py + 1, ny), lax.rem(py + ny - 1, ny)
    z_up, z_down = lax.rem(pz + 1, nz), lax.rem(pz + nz - 1, nz)
    x_mirror = nx - 1 - px
    odd = lax.rem(px, 2)
    rim = 6 * odd

    barrier = pltpu.get_barrier_semaphore()
    for device in (
        (x_up, py, pz), (x_down, py, pz),
        (px, y_up, pz), (px, y_down, pz), (x_mirror, y_up, pz), (x_mirror, y_down, pz),
        (px, py, z_up), (px, py, z_down),
    ):
        pl.semaphore_signal(barrier, inc=1, device_id=device, device_id_type=MESH)

    def load(t):
        return pltpu.make_async_copy(
            control.at[:, :, :, pl.ds(pl.multiple_of(t * LANES, LANES), LANES)],
            ubuf.at[t, :, :, pl.ds(0, 7), :],
            load_sem.at[t],
        )

    small = [
        pltpu.make_async_copy(source, target, small_sem.at[n])
        for n, source, target in (
            (0, orient_in, orient),
            (1, diag_in, raw.at[pl.ds(0, 3)]),
            (1, off_in, raw.at[pl.ds(3, 3)]),
            (1, weight_in, raw.at[6]),
            (2, forward_in, forward),
            (3, mixed_in_hbm, mixed),
            (4, plain_in_hbm, plain),
        )
    ]
    load(0).start()
    for c in small:
        c.start()
    for t in range(1, tiles):
        load(t).start()

    pad = jnp.zeros((7, 7, 1, LANES), F32)
    for t in range(tiles):
        ubuf[t, :, :, pl.ds(7, 1), :] = pad

    small[0].wait()
    pltpu.make_async_copy(raw, raw, small_sem.at[1]).wait()
    flip_i, flip_j, flip_k = (orient[0, 0, 0, d] for d in range(3))
    variant = 2 * flip_j + flip_k

    scales[pl.ds(0, 56), pl.ds(0, 64)] = raw[...].reshape(56, 64)
    turned = scales[...].T[:64]

    def spread(m):
        metric[m] = jnp.broadcast_to(turned[:, m : m + 1], (64, LANES))

    def compute(t, first=False):
        load(t).wait()
        if first:
            for c in small[4:]:
                c.wait()
        forward_table = forward[...]
        mixed_table = mixed[variant]
        plain_table = plain[variant]
        nothing = jnp.zeros((8, LANES), F32)
        def ahead(e):
            source = [ubuf[t, i].reshape(56, LANES) for i in range(e, e + 4)]
            value_cat, slope_cat = [], []
            for a in (2 * e, 2 * e + 1):
                for table, cat in ((values, value_cat), (slopes, slope_cat)):
                    x = mac([(table[a, e + n], source[n]) for n in range(4)])
                    high, low = halves(jnp.concatenate([x, nothing], axis=0))
                    cat.append(jnp.concatenate([high, high, low], axis=0))
            at_values = jnp.dot(
                forward_table, jnp.concatenate(value_cat, axis=1), preferred_element_type=F32
            )
            at_slopes = jnp.dot(
                forward_table[:64], jnp.concatenate(slope_cat, axis=1), preferred_element_type=F32
            )
            return at_values, at_slopes

        def back(e, at_values, at_slopes):
            if first:
                for m in range(7):
                    spread(8 * m + 2 * e)
                    spread(8 * m + 2 * e + 1)
            mixed_in, plain_in = [], []
            for n, a in enumerate((2 * e, 2 * e + 1)):
                lanes = slice(n * LANES, (n + 1) * LANES)
                p, g2, g3 = (at_values[64 * r : 64 * r + 64, lanes] for r in range(3))
                g1 = at_slopes[:, lanes]
                d0, d1, d2, o0, o1, o2, w = (metric[8 * s + a] for s in range(7))
                f1 = d0 * g1 + o0 * g2 + o1 * g3
                f2 = o0 * g1 + d1 * g2 + o2 * g3
                f3 = o1 * g1 + o2 * g2 + d2 * g3
                f1h, f1l = halves(f1)
                f2h, f2l = halves(f2)
                f3h, f3l = halves(f3)
                mh, ml = halves(w * p)
                mixed_in.append(jnp.concatenate([f2h, f3h, f2l, f3l], axis=0))
                plain_in.append(jnp.concatenate([f1h, f1l, mh, ml], axis=0))
            mixed_back = jnp.dot(
                mixed_table, jnp.concatenate(mixed_in, axis=1), preferred_element_type=F32
            )
            plain_back = jnp.dot(
                plain_table, jnp.concatenate(plain_in, axis=1), preferred_element_type=F32
            )
            return mixed_back, plain_back

        def gather(e, mixed_back, plain_back):
            terms = []
            for n in range(2):
                lanes = slice(n * LANES, (n + 1) * LANES)
                terms.append(
                    (
                        plain_back[0:56, lanes] + plain_back[64:120, lanes],
                        mixed_back[0:56, lanes] + mixed_back[64:120, lanes],
                        plain_back[128:184, lanes] + plain_back[192:248, lanes],
                    )
                )
            for i in range(e, e + 4):
                stiff = mac(
                    [(slopes[2 * e + n, i], terms[n][0]) for n in range(2)]
                    + [(values[2 * e + n, i], terms[n][1]) for n in range(2)]
                )
                mass = mac([(values[2 * e + n, i], terms[n][2]) for n in range(2)])
                if e > 0 and i < e + 3:
                    stiff = stiff + planes[0, i]
                    mass = mass + planes[1, i]
                planes[0, i] = stiff
                planes[1, i] = mass

        up = {e: ahead(e) for e in range(4)}
        down = {}
        for e in range(4):
            down[e] = back(e, *up.pop(e))
            if e >= 1:
                gather(e - 1, *down.pop(e - 1))
        gather(3, *down.pop(3))
        for o in range(2):
            for i in range(7):
                gbuf[o, t, i] = planes[o, i + flip_i * (6 - 2 * i)].reshape(7, 8, LANES)

    def remote(t, which, src, dst, device):
        return pltpu.make_async_remote_copy(
            src_ref=src, dst_ref=dst, send_sem=sems.at[t, which], recv_sem=sems.at[t, which],
            device_id=device, device_id_type=MESH,
        )

    rows = pl.ds(0, 7)

    def x_copies(t):
        return [
            remote(t, 0, gbuf.at[:, t, 6, :, rows, :], xrecv.at[t, 0, :, :, rows, :], (x_up, py, pz)),
            remote(t, 0, gbuf.at[:, t, 0, :, rows, :], xrecv.at[t, 1, :, :, rows, :], (x_down, py, pz)),
        ]

    def y_pair(t, which, sent, received):
        return [
            remote(t, which, sent.at[t, 1], received.at[t, 0], (px, y_up, pz)),
            remote(t, which, sent.at[t, 0], received.at[t, 1], (px, y_down, pz)),
        ]

    def y_inner(t):
        return y_pair(t, 1, ysend_inner, yrecv_inner)

    def y_ends(t):
        return y_pair(t, 2, ysend_ends, yrecv_ends)

    def y_sides(t):
        near = 6 - rim
        there = 1 - odd
        return [
            remote(t, 3, gbuf.at[:, t, near, 6, rows, :], yrecv_sides.at[t, 0, there, :, rows, :], (px, y_up, pz)),
            remote(t, 3, gbuf.at[:, t, near, 0, rows, :], yrecv_sides.at[t, 1, there, :, rows, :], (px, y_down, pz)),
            remote(t, 3, gbuf.at[:, t, rim, 6, rows, :], yrecv_sides.at[t, 0, there, :, rows, :], (x_mirror, y_up, pz)),
            remote(t, 3, gbuf.at[:, t, rim, 0, rows, :], yrecv_sides.at[t, 1, there, :, rows, :], (x_mirror, y_down, pz)),
        ]

    def z_pair(t, which, sent, received):
        return [
            remote(t, which, sent.at[t, 1], received.at[t, 0], (px, py, z_up)),
            remote(t, which, sent.at[t, 0], received.at[t, 1], (px, py, z_down)),
        ]

    def z_inner(t):
        return z_pair(t, 4, zsend_inner, zrecv_inner)

    def z_sides(t):
        return z_pair(t, 5, zsend_sides, zrecv_sides)

    def start(copies):
        for c in copies:
            c.start()

    def wait(t, which):
        views = (
            xrecv.at[pl.ds(0, 2), :, :, :, rows, :],
            yrecv_inner.at[pl.ds(0, 2)],
            yrecv_ends.at[pl.ds(0, 2)],
            yrecv_sides.at[pl.ds(0, 2), :, :, :, rows, :],
            zrecv_inner.at[pl.ds(0, 2)],
            zrecv_sides.at[pl.ds(0, 2)],
        )
        pltpu.make_async_copy(views[which], views[which], sems.at[t, which]).wait()

    def fold_x(t):
        for side in range(2):
            for o in range(2):
                gbuf[o, t, 6 * side, :, rows, :] = (
                    gbuf[o, t, 6 * side, :, rows, :] + xrecv[t, side, o, :, rows, :]
                )

    inner_rows = [(i, i - 1) for i in range(1, 6)]
    side_rows = [(6 * n, n) for n in range(2)]

    def take_z(t, sent, where):
        for side in range(2):
            for o in range(2):
                for i, n in where:
                    sent[t, side, o, n] = gbuf[o, t, i, :, 6 * side, :]

    def fold_z(t, received, where):
        for side in range(2):
            for o in range(2):
                for i, n in where:
                    gbuf[o, t, i, :, 6 * side, :] = gbuf[o, t, i, :, 6 * side, :] + received[t, side, o, n]

    mid = pl.ds(1, 5)

    def take_y_inner(t):
        for side in range(2):
            for o in range(2):
                ysend_inner[t, side, o] = gbuf[o, t, mid, 6 * side, mid, :]

    def take_y_ends(t):
        for side in range(2):
            for o in range(2):
                for n in range(2):
                    ysend_ends[t, side, o, n] = gbuf[o, t, mid, 6 * side, 6 * n, :]

    def fold_y(t):
        for side in range(2):
            for o in range(2):
                j = 6 * side
                gbuf[o, t, mid, j, mid, :] = gbuf[o, t, mid, j, mid, :] + yrecv_inner[t, side, o]
                for n in range(2):
                    gbuf[o, t, mid, j, 6 * n, :] = gbuf[o, t, mid, j, 6 * n, :] + yrecv_ends[t, side, o, n]
                    gbuf[o, t, 6 * n, j, rows, :] = gbuf[o, t, 6 * n, j, rows, :] + yrecv_sides[t, side, n, o, rows, :]

    sublane = lax.broadcasted_iota(jnp.int32, (8, LANES), 0)
    turned_rows = jnp.where(sublane < 7, 6 - sublane, sublane)
    pick = sublane + flip_k * (turned_rows - sublane)

    def finish(t):
        lanes = pl.ds(pl.multiple_of(t * LANES, LANES), LANES)
        for o, out in enumerate((stiff_out, mass_out)):
            for i in range(7):
                for j in range(7):
                    tile = gbuf[o, t, i + flip_i * (6 - 2 * i), j + flip_j * (6 - 2 * j)]
                    out[i, j, :, lanes] = jnp.take_along_axis(tile, pick, axis=0)[:7]

    def send_first(t):
        start(x_copies(t))
        take_z(t, zsend_inner, inner_rows)
        start(z_inner(t))
        take_y_inner(t)

    def produce(t, carry):
        compute(t)
        send_first(t)
        start(y_inner(t - 1))
        return carry

    def after_x(t, carry):
        wait(t, 0)
        fold_x(t)
        take_z(t, zsend_sides, side_rows)
        start(z_sides(t))
        return carry

    def after_z(t, carry):
        wait(t, 4)
        fold_z(t, zrecv_inner, inner_rows)
        take_y_ends(t)
        start(y_ends(t))
        wait(t, 5)
        fold_z(t, zrecv_sides, side_rows)
        start(y_sides(t))
        return carry

    def after_y(t, carry):
        wait(t, 1)
        wait(t, 2)
        wait(t, 3)
        fold_y(t)
        finish(t)
        return carry

    compute(0, first=True)
    pl.semaphore_wait(barrier, 8)
    send_first(0)
    lax.fori_loop(1, tiles, produce, 0)
    start(y_inner(tiles - 1))
    for stage in (after_x, after_z, after_y):
        lax.fori_loop(0, tiles, stage, 0)


def put(stiff, mass, stiff_out, mass_out, sem):
    copies = [
        pltpu.make_async_copy(source, target, sem.at[n])
        for n, (source, target) in enumerate(((stiff, stiff_out), (mass, mass_out)))
    ]
    for c in copies:
        c.start()
    for c in copies:
        c.wait()


def per_device(control_values, metric_diag, metric_off, mass_weight, orient):
    values, slopes = spline_tables(4)
    tiles = control_values.shape[-1] // LANES
    forward, mixed, plain = (jnp.asarray(t) for t in matmul_tables(values, slopes))
    shape = jax.ShapeDtypeStruct(control_values.shape, F32)
    in_vmem = pl.BlockSpec(memory_space=pltpu.VMEM)
    in_hbm = pl.BlockSpec(memory_space=pltpu.HBM)
    results = pl.pallas_call(
        functools.partial(kernel, values, slopes, tiles),
        out_shape=(pltpu.VMEM(control_values.shape, F32),) * 2,
        in_specs=[in_hbm] * 8,
        out_specs=(in_vmem, in_vmem),
        scratch_shapes=[
            pltpu.VMEM((7, 8, 64), F32),
            pltpu.SMEM(orient.shape, jnp.int32),
            pltpu.VMEM(forward.shape, BF16),
            pltpu.VMEM(mixed.shape, BF16),
            pltpu.VMEM(plain.shape, BF16),
            pltpu.VMEM((tiles, 7, 7, 8, LANES), F32),
            pltpu.VMEM((2, tiles, 7, 7, 8, LANES), F32),
            pltpu.VMEM((2, 7, 56, LANES), F32),
            pltpu.VMEM((56, 64, LANES), F32),
            pltpu.VMEM((128, 128), F32),
            pltpu.VMEM((tiles, 2, 2, 7, 8, LANES), F32),
            pltpu.VMEM((tiles, 2, 2, 5, 5, LANES), F32),
            pltpu.VMEM((tiles, 2, 2, 5, 5, LANES), F32),
            pltpu.VMEM((tiles, 2, 2, 2, 5, LANES), F32),
            pltpu.VMEM((tiles, 2, 2, 2, 5, LANES), F32),
            pltpu.VMEM((tiles, 2, 2, 2, 8, LANES), F32),
            pltpu.VMEM((tiles, 2, 2, 5, 7, LANES), F32),
            pltpu.VMEM((tiles, 2, 2, 5, 7, LANES), F32),
            pltpu.VMEM((tiles, 2, 2, 2, 7, LANES), F32),
            pltpu.VMEM((tiles, 2, 2, 2, 7, LANES), F32),
            pltpu.SemaphoreType.DMA((tiles,)),
            pltpu.SemaphoreType.DMA((5,)),
            pltpu.SemaphoreType.DMA((tiles, 6)),
        ],
        compiler_params=pltpu.CompilerParams(
            collective_id=0, has_side_effects=True, vmem_limit_bytes=40 * 1024 * 1024
        ),
        name="apply",
    )(
        *(
            pltpu.with_memory_space_constraint(x, pltpu.HBM)
            for x in (control_values, metric_diag, metric_off, mass_weight, orient, forward, mixed, plain)
        )
    )
    return pl.pallas_call(
        put,
        out_shape=(shape, shape),
        in_specs=[pl.BlockSpec(memory_space=pl.ANY)] * 2,
        out_specs=(in_hbm, in_hbm),
        scratch_shapes=[pltpu.SemaphoreType.DMA((2,))],
        compiler_params=pltpu.CompilerParams(vmem_limit_bytes=1024 * 1024),
        name="put",
    )(*(pltpu.with_memory_space_constraint(x, pltpu.VMEM) for x in results))


def solution(mesh):
    in_specs = (
        P("px", "py", "pz", None),
        P(None, "px", ("py", "pz")),
        P(None, "px", ("py", "pz")),
        P("px", ("py", "pz")),
        P("px", "py", "pz", None),
    )
    out_specs = (P("px", "py", "pz", None), P("px", "py", "pz", None))
    return jax.shard_map(
        per_device, mesh=mesh, in_specs=in_specs, out_specs=out_specs, check_vma=False
    )
```
